256 devices in a mesh: groups: 2 (over y), ep: 32 (over z, core), sub: 4 (over x).
Axes of the slice: x: 4, y: 2, z: 16, core: 2. Of those that a mesh axis runs over, the one named last changes fastest.
The devices are a block of a 4x16x16 slice.
Arguments:
- tokens: bfloat16 [4096, 7168], P(('groups', 'ep'), 'sub'), parts along dimension 0, may hold values from -6 to 6
- expert_ids: int32 [4096, 8], P(('groups', 'ep')), parts along dimension 0, may hold values from 0 to 31, all different within a row; in each aligned block of 64 rows (0 to 63, 64 to 127, ...) at most 24 rows name the same one
- route_weights: float32 [4096, 8], P(('groups', 'ep')), parts along dimension 0, may hold values from 0.05 to 0.6
- gate_weight: bfloat16 [32, 7168, 1024], P('ep', 'sub'), may hold values from -0.0625 to 0.0625
- up_weight: bfloat16 [32, 7168, 1024], P('ep', 'sub'), may hold values from -0.0625 to 0.0625
- down_weight: bfloat16 [32, 1024, 7168], P('ep', None, 'sub'), may hold values from -0.1875 to 0.1875
- shared_gate: bfloat16 [1024, 7168], P('ep', 'sub'), may hold values from -0.0625 to 0.0625
- shared_up: bfloat16 [1024, 7168], P('ep', 'sub'), may hold values from -0.0625 to 0.0625
- shared_down: bfloat16 [1024, 7168], P('ep', 'sub'), may hold values from -0.1875 to 0.1875
Outputs:
- layer_out: bfloat16 [4096, 7168], P(('groups', 'ep'), 'sub'), parts along dimension 0
The draws below stay inside these ranges and needn't reach their ends.
There are 2 independent parts, one for each index of `groups`. The reference program is written for one: setup_inputs(seed, part) draws one part's arguments, and reference() takes and returns one part's arrays. A program takes and returns all parts, laid end to end along the dimension named above; an argument that names none is the same for every part. Nothing has to cross between parts.
Inputs may be any that keep to these rules, and one draw needn't show every extreme that they name: `expert_ids`: each row names 8 different experts. Among the 64 rows of one ep index no expert is named more than 24 times, and in some of these aligned blocks an expert is named exactly 24 times.
All inputs are finite; a program needn't handle non-finite values.
Results may differ from the reference program's by a relative error of at most 0.0054.
Values may be sent and summed in bfloat16 or wider, within the bound.
A program may use at most 128 MiB of HBM per device.

```python
import math
import jax
import jax.numpy as jnp
import numpy as np
from jax import lax

D = 7168
HIDDEN_SIZE = 1024
SH = 1024
TOK_EP = 64
EXPERTS = 32
TOPK = 8
CAP = 24
TOKENS = 2048
N_EP = 32


def level_of(stream_key, shape, pieces, least, largest):
    def one(dim, shards_of):
        steps = jax.random.uniform(jax.random.fold_in(jax.random.fold_in(stream_key, 6), dim), (shards_of,), jnp.float32, least / len(pieces), largest / len(pieces))
        return jnp.repeat(jnp.exp(steps), shape[dim] // shards_of).reshape((-1,) + (1,) * (len(shape) - dim - 1))

    gain = one(*pieces[0])
    for cut in pieces[1:]:
        gain = gain * one(*cut)
    return gain


def deal_out(stream_key, own, number, rows, count, top, limit, lean):
    order = jax.random.permutation(stream_key, count)
    heavy_load, ordinary = portions_of(count, rows * top, limit, lean, True), portions_of(count, rows * top, limit, lean, False)
    places = jnp.arange(count)

    def named(lengths, offset_by):
        used = int((lengths > 0).sum())
        fixed = max(1, used // 4)
        moved = fixed + (places - fixed + offset_by * (used - fixed)) % max(1, count - fixed)
        return jnp.zeros((count,), jnp.int32).at[order[jnp.where(places < fixed, places, moved)]].set(jnp.asarray(lengths, jnp.int32))

    lengths = jnp.where(number % 4 == 0, named(heavy_load, number // 4), named(ordinary, number - number // 4 - 1))
    mixed = jax.random.permutation(jax.random.fold_in(own, 3), count)
    giver, sink = mixed[0:count // 2 * 2:2], mixed[1:count // 2 * 2:2]
    slack = jnp.minimum(lengths[giver] - 1, limit - lengths[sink]) // 2
    slack = jnp.where((giver == order[0]) | (sink == order[0]) | (lengths[sink] == 0), 0, jnp.maximum(slack, 0))
    moved = jax.random.randint(jax.random.fold_in(own, 4), (count // 2,), 0, 1 << 20) % (slack + 1)
    lengths = lengths.at[giver].add(-moved).at[sink].add(moved)
    labels = jnp.searchsorted(jnp.cumsum(lengths), jnp.arange(rows * top), side="right").astype(jnp.int32)
    grid = labels.reshape(top, rows).T
    grid = grid[jax.random.permutation(jax.random.fold_in(own, 1), rows)]
    offset_by = jax.random.randint(jax.random.fold_in(own, 2), (rows, 1), 0, top)
    return jnp.take_along_axis(grid, (jnp.arange(top)[None, :] + offset_by) % top, axis=1)


def portions_of(number_of, total, bound, lean, full):
    loads = [(1 << 20) // math.isqrt(rank ** lean) + 1 for rank in range(1, number_of + 1)]
    largest = bound if full else min(bound, max(-(-total // number_of), total * loads[0] // sum(loads)))
    least = 1 if total - largest >= number_of - 1 else 0
    counts, spare = [largest] + [least] * (number_of - 1), total - largest - least * (number_of - 1)
    while spare > 0:
        movable = [i for i in range(1, number_of) if counts[i] < largest] or [i for i in range(1, number_of) if counts[i] < bound]
        mass, left = sum([loads[i] for i in movable]), spare
        for i in movable:
            extra = min(bound - counts[i], max(1, left * loads[i] // mass), spare)
            counts[i] = counts[i] + extra
            spare = spare - extra
    return np.array(counts)


def centred(stream_key, extent, width, reach, split=(), kind=jnp.bfloat16):
    gain = level_of(stream_key, extent, split, -0.22, 0.18) if split else 1.0
    values = jax.random.normal(stream_key, extent, jnp.float32) * width * gain
    return jnp.minimum(jnp.maximum(values, -reach), reach).astype(kind)


def setup_inputs(seed: int = 0, part: int = 0) -> dict:
    key_of = jax.random.split(jax.random.key(seed), 10)
    part_keys = jax.random.split(jax.random.fold_in(key_of[9], part), 10)
    tokens = centred(part_keys[0], (TOKENS, D), 1.0, 6.0, ((0, 32), (1, 4)))
    expert_ids_keys = jax.random.split(jax.random.fold_in(part_keys[1], 1), TOKENS // TOK_EP)
    expert_ids_turns = jax.random.permutation(jax.random.fold_in(part_keys[1], 3), TOKENS // TOK_EP)
    expert_ids = jax.vmap(lambda own, number: deal_out(jax.random.fold_in(part_keys[1], 2), own, number, TOK_EP, EXPERTS, TOPK, CAP, 2))(expert_ids_keys, expert_ids_turns).reshape((TOKENS, TOPK))
    route_weights = jnp.clip(jnp.exp(math.log(0.6) - 2.4849067 * jax.random.uniform(part_keys[2], (TOKENS, TOPK), jnp.float32) ** level_of(part_keys[2], (TOKENS, TOPK), ((0, 32),), -0.2, 0.2)), 0.05, 0.6)
    gate_weight = centred(key_of[3], (EXPERTS, D, HIDDEN_SIZE), D ** -0.5, 0.0625, ((0, 32), (1, 4)))
    up_weight = centred(key_of[4], (EXPERTS, D, HIDDEN_SIZE), D ** -0.5, 0.0625, ((0, 32), (1, 4)))
    down_weight = centred(key_of[5], (EXPERTS, HIDDEN_SIZE, D), HIDDEN_SIZE ** -0.5, 0.1875, ((0, 32), (2, 4)))
    shared_gate = centred(key_of[6], (SH, D), D ** -0.5, 0.0625, ((0, 32), (1, 4)))
    shared_up = centred(key_of[7], (SH, D), D ** -0.5, 0.0625, ((0, 32), (1, 4)))
    shared_down = centred(key_of[8], (SH, D), SH ** -0.5, 0.1875, ((0, 32), (1, 4)))
    return {"tokens": tokens, "expert_ids": expert_ids, "route_weights": route_weights, "gate_weight": gate_weight, "up_weight": up_weight, "down_weight": down_weight, "shared_gate": shared_gate, "shared_up": shared_up, "shared_down": shared_down}


def reference(tokens, expert_ids, route_weights, gate_weight, up_weight, down_weight, shared_gate, shared_up, shared_down):
    contract = (((1,), (1,)), ((), ()))
    shared_pre = lax.dot_general(tokens, shared_gate, contract, preferred_element_type=jnp.float32)
    shared_lin = lax.dot_general(tokens, shared_up, contract, preferred_element_type=jnp.float32)
    shared_hidden = (jax.nn.silu(shared_pre) * shared_lin).astype(jnp.bfloat16)
    shared_out = jnp.dot(shared_hidden, shared_down, preferred_element_type=jnp.float32)
    most_rows = N_EP * CAP

    def expert_step(totals, inputs):
        gate_mat, up_mat, down_mat, expert = inputs
        chosen = expert_ids == expert
        weight_col = jnp.sum(jnp.where(chosen, route_weights, jnp.float32(0.0)), axis=1)
        absent = 1 - jnp.any(chosen, axis=1).astype(jnp.int32)
        row_order = jnp.argsort(absent, stable=True)[:most_rows].astype(jnp.int32)
        picked = tokens[row_order]
        expert_pre = jnp.dot(picked, gate_mat, preferred_element_type=jnp.float32)
        expert_lin = jnp.dot(picked, up_mat, preferred_element_type=jnp.float32)
        expert_hidden = (jax.nn.silu(expert_pre) * expert_lin).astype(jnp.bfloat16)
        expert_out = jnp.dot(expert_hidden, down_mat, preferred_element_type=jnp.float32).astype(jnp.bfloat16)
        totals = totals.at[row_order].add(weight_col[row_order][:, None] * expert_out.astype(jnp.float32))
        return totals, None

    expert_index = jnp.arange(EXPERTS, dtype=jnp.int32)
    routed, unused = lax.scan(expert_step, jnp.zeros((TOKENS, D), jnp.float32), (gate_weight, up_weight, down_weight, expert_index))
    return (shared_out + routed).astype(jnp.bfloat16)
```

```python
import functools

import jax
import jax.numpy as jnp
from jax import lax
from jax.experimental import pallas as pl
from jax.experimental.pallas import tpu as pltpu
from jax.sharding import PartitionSpec as P

MESH = pl.DeviceIdType.MESH
NC = 4


def layer_kernel(
    dims,
    tokens_ref,
    meta_ref,
    sgate_ref,
    sup_ref,
    sdown_ref,
    gate_hbm,
    up_hbm,
    down_hbm,
    out_ref,
    gate_v,
    up_v,
    down_v,
    tok,
    meta,
    comp,
    upper,
    lhs_t,
    wsel,
    xs,
    xr1,
    xc,
    xr2,
    ss,
    sr1,
    sc,
    sr2,
    hid,
    hsb,
    con,
    ps,
    pr,
    rs_s,
    rs_r,
    w_sem,
    ag_ss,
    ag_rs,
    dd_ss,
    dd_rs,
    x1_ss,
    x1_rs,
    x2_ss,
    x2_rs,
    h1_ss,
    h1_rs,
    h2_ss,
    h2_rs,
    pd_ss,
    pd_rs,
    r_ss,
    r_rs,
):
    nz, nsub, cap, units = dims
    f32, bf16 = jnp.float32, jnp.bfloat16
    H = nz // 2
    T, Q = tokens_ref.shape
    CH = T // NC
    R = 4 * cap
    HQ = gate_v.shape[1] // nsub
    UQ = units // nsub
    TILE = 256
    ntile = Q // TILE

    e = lax.axis_index("ep")
    s = lax.axis_index("sub")
    z = e // 2
    c = e % 2
    z_right = {"ep": ((z + 1) % nz) * 2 + c}
    z_left = {"ep": ((z + nz - 1) % nz) * 2 + c}
    z_next = (z_right, z_left)
    partner = {"ep": z * 2 + (1 - c)}
    xR = (s + 1) % nsub
    xL = (s + nsub - 1) % nsub
    xO = (s + 2) % nsub
    x_right = {"sub": xR}
    x_left = {"sub": xL}

    def remote(src, dst, ssem, rsem, dev):
        return pltpu.make_async_remote_copy(
            src_ref=src, dst_ref=dst, send_sem=ssem, recv_sem=rsem, device_id=dev, device_id_type=MESH
        )

    weights = [
        pltpu.make_async_copy(a, b, w_sem.at[n])
        for n, (a, b) in enumerate(((gate_hbm, gate_v), (up_hbm, up_v), (down_hbm, down_v)))
    ]
    for w in weights:
        w.start()

    barrier = pltpu.get_barrier_semaphore()
    for peer in (z_right, z_left, partner, x_right, x_left):
        pl.semaphore_signal(barrier, inc=1, device_id=peer, device_id_type=MESH)
    pl.semaphore_wait(barrier, 5)

    def mine(m, i):
        return (i < NC // 2 or i == NC) if m == 0 else (NC // 2 <= i < NC)

    def slot_of(m, t):
        return m * (1 - t // H)

    def rows_of(d, rel, i):
        return pl.ds((2 * d + rel) * T + i * CH, CH)

    def ring(m, t, i, first=False):
        d = slot_of(m, t)
        if i == NC:
            src = meta_ref if first else meta.at[t - 2, 2 * m]
            dst = meta.at[t - 1, 2 * d]
        else:
            src = tokens_ref.at[pl.ds(i * CH, CH)] if first else tok.at[t - 2, rows_of(m, 0, i)]
            dst = tok.at[t - 1, rows_of(d, 0, i)]
        return remote(src, dst, ag_ss.at[m, t - 1, i], ag_rs.at[m, t - 1, i], z_next[m])

    def ring_arrival(m, t, i):
        d = slot_of(m, t)
        dst = meta.at[t - 1, 2 * d] if i == NC else tok.at[t - 1, rows_of(d, 0, i)]
        return remote(dst, dst, ag_ss.at[m, t - 1, i], ag_rs.at[m, t - 1, i], z_next[m])

    def hand(d, t, i, own=False):
        if i == NC:
            src = meta_ref if own else meta.at[t - 1, 2 * d]
            dst = meta.at[t - 1, 2 * d + 1]
        else:
            src = tokens_ref.at[pl.ds(i * CH, CH)] if own else tok.at[t - 1, rows_of(d, 0, i)]
            dst = tok.at[t - 1, rows_of(d, 1, i)]
        return remote(src, dst, dd_ss.at[d, t - 1, i], dd_rs.at[d, t - 1, i], partner)

    order = [0, NC] + list(range(1, NC))
    for i in order:
        for m in (0, 1):
            if H > 1 or mine(m, i):
                ring(m, 1, i, first=True).start()
    for i in order:
        hand(1, H, i, own=True).start()
    tok[H - 1, 2 * T : 3 * T, :] = tokens_ref[...]
    meta[H - 1, 2] = meta_ref[...]

    row_i = lax.broadcasted_iota(jnp.int32, (4 * T, 4 * T), 0)
    col_i = lax.broadcasted_iota(jnp.int32, (4 * T, 4 * T), 1)
    upper[...] = ((row_i < col_i) & (row_i // T == col_i // T)).astype(f32).astype(bf16)

    def forward(t, i):
        for m in (0, 1):

            @pl.when(t < H)
            def _():
                ring_arrival(m, t, i).wait_recv()
                if mine(m, i):
                    ring(m, t + 1, i).start()
                else:

                    @pl.when(t + 1 < H)
                    def _():
                        ring(m, t + 1, i).start()

                hand(m, t, i).start()

            if mine(m, i):

                @pl.when(t == H)
                def _():
                    ring_arrival(m, t, i).wait_recv()
                    hand(0, t, i).start()

    def stage1a(k):
        for d in (0, 1):
            for i in range(NC + 1):
                hand(d, k, i).wait_recv()
        half = lax.broadcasted_iota(jnp.int32, meta_ref.shape, 1) < T
        ids, ws = [], []
        for d in (0, 1):
            m0 = meta[k - 1, 2 * d]
            m1 = meta[k - 1, 2 * d + 1]
            ids.append(jnp.where(half, m0, pltpu.roll(m1, T, 1)))
            ws.append(jnp.where(half, pltpu.roll(m0, T, 1), m1))
        ids = jnp.concatenate(ids, axis=1)
        ws = jnp.concatenate(ws, axis=1)
        hit = ids == e.astype(f32)
        sel = jnp.max(jnp.where(hit, 1.0, 0.0), axis=0, keepdims=True)
        wsel[k - 1] = jnp.broadcast_to(
            jnp.sum(jnp.where(hit, ws, 0.0), axis=0, keepdims=True), (8, 4 * T)
        )
        sel8 = jnp.broadcast_to(sel, (16, 4 * T)).astype(bf16)
        pos = jnp.dot(sel8, upper[...], preferred_element_type=f32)[0:1]
        base = (lax.broadcasted_iota(jnp.int32, (1, 4 * T), 1) // T * cap).astype(f32)
        target = jnp.where(sel > 0.0, pos + base, -1.0)
        place = lax.broadcasted_iota(jnp.int32, (R, 4 * T), 0).astype(f32) == target
        place = jnp.where(place, 1.0, 0.0).astype(bf16)
        lhs_t[k - 1, 0:R, :] = place

        def pick(n, _):
            cols = pl.ds(pl.multiple_of(n * TILE, TILE), TILE)
            comp[:, cols] = jnp.dot(place, tok[k - 1, :, cols], preferred_element_type=f32).astype(bf16)
            return 0

        lax.fori_loop(0, ntile, pick, 0)

    def x_first(k):
        return (
            remote(xs.at[k - 1, xO, 0], xr1.at[k - 1, 0], x1_ss.at[k - 1, 0], x1_rs.at[k - 1, 0], x_right),
            remote(xs.at[k - 1, xO, 1], xr1.at[k - 1, 2], x1_ss.at[k - 1, 2], x1_rs.at[k - 1, 2], x_left),
            remote(ss.at[k - 1, xO, 0], sr1.at[k - 1, 0], x1_ss.at[k - 1, 4], x1_rs.at[k - 1, 4], x_right),
            remote(ss.at[k - 1, xO, 1], sr1.at[k - 1, 2], x1_ss.at[k - 1, 6], x1_rs.at[k - 1, 6], x_left),
            remote(xs.at[k - 1, xR, 1], xr1.at[k - 1, 1], x1_ss.at[k - 1, 1], x1_rs.at[k - 1, 1], x_right),
            remote(xs.at[k - 1, xL, 0], xr1.at[k - 1, 3], x1_ss.at[k - 1, 3], x1_rs.at[k - 1, 3], x_left),
            remote(ss.at[k - 1, xR, 1], sr1.at[k - 1, 1], x1_ss.at[k - 1, 5], x1_rs.at[k - 1, 5], x_right),
            remote(ss.at[k - 1, xL, 0], sr1.at[k - 1, 3], x1_ss.at[k - 1, 7], x1_rs.at[k - 1, 7], x_left),
        )

    def stage1b(k):
        rows = comp[...]

        def project(j, _):
            cols = pl.ds(pl.multiple_of(j * HQ, HQ), HQ)
            xs[k - 1, j, 0] = jnp.dot(rows, gate_v[:, cols], preferred_element_type=f32).astype(bf16)
            xs[k - 1, j, 1] = jnp.dot(rows, up_v[:, cols], preferred_element_type=f32).astype(bf16)
            return 0

        lax.fori_loop(0, nsub, project, 0)
        contract = (((1,), (1,)), ((), ()))
        pre = lax.dot_general(sgate_ref[...], tok[k - 1], contract, preferred_element_type=f32)
        lin = lax.dot_general(sup_ref[...], tok[k - 1], contract, preferred_element_type=f32)
        for j in range(nsub):
            ss[k - 1, j, 0] = pre[j * UQ : (j + 1) * UQ]
            ss[k - 1, j, 1] = lin[j * UQ : (j + 1) * UQ]
        for copy in x_first(k):
            copy.start()

    def x_second(k):
        return (
            remote(xc.at[k - 1, 0], xr2.at[k - 1, 0], x2_ss.at[k - 1, 0], x2_rs.at[k - 1, 0], x_right),
            remote(xc.at[k - 1, 1], xr2.at[k - 1, 1], x2_ss.at[k - 1, 1], x2_rs.at[k - 1, 1], x_left),
            remote(sc.at[k - 1, 0], sr2.at[k - 1, 0], x2_ss.at[k - 1, 2], x2_rs.at[k - 1, 2], x_right),
            remote(sc.at[k - 1, 1], sr2.at[k - 1, 1], x2_ss.at[k - 1, 3], x2_rs.at[k - 1, 3], x_left),
        )

    def stage2(k):
        first = x_first(k)
        second = x_second(k)
        for m, toward in ((0, xR), (1, xL)):
            first[m].wait_recv()
            xc[k - 1, m] = (
                xs[k - 1, toward, m].astype(f32) + xr1[k - 1, 2 * m].astype(f32)
            ).astype(bf16)
            second[m].start()
        for m, toward in ((0, xR), (1, xL)):
            first[2 + m].wait_recv()
            sc[k - 1, m] = ss[k - 1, toward, m] + sr1[k - 1, 2 * m]
            second[2 + m].start()

    own_cols = pl.ds(pl.multiple_of(s * HQ, HQ), HQ)
    left_cols = pl.ds(pl.multiple_of(xL * HQ, HQ), HQ)
    right_cols = pl.ds(pl.multiple_of(xR * HQ, HQ), HQ)
    far_cols = pl.ds(pl.multiple_of(xO * HQ, HQ), HQ)
    own_rows = pl.ds(pl.multiple_of(s * UQ, UQ), UQ)
    left_rows = pl.ds(pl.multiple_of(xL * UQ, UQ), UQ)
    right_rows = pl.ds(pl.multiple_of(xR * UQ, UQ), UQ)
    far_rows = pl.ds(pl.multiple_of(xO * UQ, UQ), UQ)

    def h_copy(k, n, cols, rows, dev):
        view = hid.at[k - 1, :, cols]
        small = hsb.at[k - 1, rows, :]
        return (
            remote(view, view, h1_ss.at[k - 1, n], h1_rs.at[k - 1, n], dev),
            remote(small, small, h1_ss.at[k - 1, 2 + n], h1_rs.at[k - 1, 2 + n], dev),
        )

    def stage3(k):
        for copy in x_first(k)[4:]:
            copy.wait_recv()
        for copy in x_second(k):
            copy.wait_recv()
        gate = xs[k - 1, s, 0].astype(f32) + xr1[k - 1, 3].astype(f32) + xr2[k - 1, 0].astype(f32)
        up = xs[k - 1, s, 1].astype(f32) + xr1[k - 1, 1].astype(f32) + xr2[k - 1, 1].astype(f32)
        hid[k - 1, :, own_cols] = (gate / (1.0 + jnp.exp(-gate)) * up).astype(bf16)
        sg = ss[k - 1, s, 0] + sr1[k - 1, 3] + sr2[k - 1, 0]
        su = ss[k - 1, s, 1] + sr1[k - 1, 1] + sr2[k - 1, 1]
        hsb[k - 1, own_rows, :] = sg / (1.0 + jnp.exp(-sg)) * su
        for copy in h_copy(k, 0, own_cols, own_rows, x_right) + h_copy(k, 1, own_cols, own_rows, x_left):
            copy.start()

    def h_far(k, n, cols, rows, dev):
        view = hid.at[k - 1, pl.ds(n * (R // 2), R // 2), cols]
        small = hsb.at[k - 1, rows, pl.ds(n * 2 * T, 2 * T)]
        return (
            remote(view, view, h2_ss.at[k - 1, n], h2_rs.at[k - 1, n], dev),
            remote(small, small, h2_ss.at[k - 1, 2 + n], h2_rs.at[k - 1, 2 + n], dev),
        )

    def stage4(k):
        for n, cols, rows, dev in ((0, left_cols, left_rows, x_right), (1, right_cols, right_rows, x_left)):
            for copy in h_copy(k, n, cols, rows, dev):
                copy.wait_recv()
            for copy in h_far(k, n, cols, rows, dev):
                copy.start()

    def give(k, d):
        return remote(ps.at[k - 1, d], pr.at[k - 1, d], pd_ss.at[k - 1, d], pd_rs.at[k - 1, d], partner)

    def stage5(k):
        for n, dev in ((0, x_right), (1, x_left)):
            for copy in h_far(k, n, far_cols, far_rows, dev):
                copy.wait_recv()
        lhs_t[k - 1, R : R + units, :] = hsb[k - 1].astype(bf16)
        both_t = lhs_t[k - 1]
        weight = jnp.sum(both_t[0:R].astype(f32) * wsel[k - 1, 0:1], axis=1, keepdims=True)
        both = jnp.transpose(both_t.astype(f32)).astype(bf16)
        hidden = hid[k - 1]

        def columns(n, _):
            cols = pl.ds(pl.multiple_of(n * TILE, TILE), TILE)
            o = jnp.dot(hidden, down_v[:, cols], preferred_element_type=f32)
            o = (o * weight).astype(bf16)
            stacked = jnp.concatenate([o, sdown_ref[:, cols]], axis=0)
            part = jnp.dot(both, stacked, preferred_element_type=f32)
            for d in (0, 1):
                con[k - 1, d, :, cols] = part[2 * d * T : (2 * d + 1) * T]
                ps[k - 1, d, :, cols] = part[(2 * d + 1) * T : (2 * d + 2) * T].astype(bf16)
            return 0

        lax.fori_loop(0, ntile, columns, 0)
        for d in (0, 1):
            give(k, d).start()

    def during(k, stage):
        @pl.when((k >= 1) & (k <= H))
        def _():
            stage(k)

    def step(t, _):
        forward(t, 0)
        forward(t, NC)

        @pl.when(t == 2)
        def _():
            for w in weights:
                w.wait()

        during(t - 1, stage1a)
        forward(t, 1)
        during(t - 1, stage1b)
        forward(t, 2)
        during(t - 5, stage5)
        forward(t, 3)
        during(t - 4, stage4)
        during(t - 3, stage3)
        during(t - 2, stage2)
        return 0

    lax.fori_loop(1, H + 6, step, 0)

    def rows(i):
        return pl.ds(i * CH, CH)

    def pass_on(m, d, i):
        return remote(
            rs_s.at[m, d - 1, rows(i)],
            rs_r.at[m, d - 1, rows(i)],
            r_ss.at[m, d - 1, i],
            r_rs.at[m, d - 1, i],
            z_next[m],
        )

    def own_sum(d, slot, i):
        return con[d - 1, slot, rows(i), :] + pr[d - 1, slot, rows(i), :].astype(f32)

    give(H, 0).wait_recv()
    for i in range(NC):
        m = 0 if mine(0, i) else 1
        rs_s[m, H - 1, rows(i), :] = own_sum(H, 0, i).astype(bf16)
        pass_on(m, H, i).start()

    def back(d, partly):
        give(d, 0).wait_recv()
        give(d, 1).wait_recv()
        for i in range(NC):
            for m in (0, 1):
                total = own_sum(d, 1 - m, i)
                if not partly or mine(m, i):
                    pass_on(m, d + 1, i).wait_recv()
                    total = total + rs_r[m, d, rows(i), :].astype(f32)
                rs_s[m, d - 1, rows(i), :] = total.astype(bf16)
                pass_on(m, d, i).start()

    if H > 1:
        back(H - 1, True)

    def back_step(n, _):
        back(H - 2 - n, False)
        return 0

    lax.fori_loop(0, H - 2, back_step, 0)
    give(H, 1).wait_recv()
    for i in range(NC):
        total = own_sum(H, 1, i)
        for m in (0, 1):
            pass_on(m, 1, i).wait_recv()
            total = total + rs_r[m, 0, rows(i), :].astype(f32)
        out_ref[rows(i), :] = total.astype(bf16)

    def drain(k, _):
        for i in range(NC + 1):
            for m in (0, 1):
                hand(m, k, i).wait_send()

                @pl.when(k < H)
                def _():
                    ring_arrival(m, k, i).wait_send()

                if mine(m, i):

                    @pl.when(k == H)
                    def _():
                        ring_arrival(m, k, i).wait_send()

        for copy in x_first(k) + x_second(k):
            copy.wait_send()
        for n, dev in ((0, x_right), (1, x_left)):
            for copy in h_copy(k, n, own_cols, own_rows, dev) + h_far(k, n, own_cols, own_rows, dev):
                copy.wait_send()
            give(k, n).wait_send()
        for i in range(NC):
            for m in (0, 1):

                @pl.when(k < H)
                def _():
                    pass_on(m, k, i).wait_send()

                if mine(m, i):

                    @pl.when(k == H)
                    def _():
                        pass_on(m, k, i).wait_send()

        return 0

    lax.fori_loop(1, H + 1, drain, 0)


def per_device(
    tokens,
    expert_ids,
    route_weights,
    gate_weight,
    up_weight,
    down_weight,
    shared_gate,
    shared_up,
    shared_down,
):
    f32, bf16 = jnp.float32, jnp.bfloat16
    nep = lax.axis_size("ep")
    nsub = lax.axis_size("sub")
    nz = nep // 2
    H = nz // 2
    T, Q = tokens.shape
    top = expert_ids.shape[1]
    cap = T * top * 3 // (2 * nep)
    units = shared_gate.shape[0]
    hidden = gate_weight.shape[2]
    HQ, UQ, R = hidden // nsub, units // nsub, 4 * cap
    meta = jnp.concatenate([expert_ids.T.astype(f32), route_weights.T], axis=1)
    vmem = pltpu.VMEM
    dma = pltpu.SemaphoreType.DMA
    vspec = pl.BlockSpec(memory_space=pltpu.VMEM)
    hspec = pl.BlockSpec(memory_space=pl.ANY)
    scratch = [
        vmem((Q, hidden), bf16),
        vmem((Q, hidden), bf16),
        vmem((hidden, Q), bf16),
        vmem((H, 4 * T, Q), bf16),
        vmem((H, 4, top, 2 * T), f32),
        vmem((R, Q), bf16),
        vmem((4 * T, 4 * T), bf16),
        vmem((H, R + units, 4 * T), bf16),
        vmem((H, 8, 4 * T), f32),
        vmem((H, nsub, 2, R, HQ), bf16),
        vmem((H, 4, R, HQ), bf16),
        vmem((H, 2, R, HQ), bf16),
        vmem((H, 2, R, HQ), bf16),
        vmem((H, nsub, 2, UQ, 4 * T), f32),
        vmem((H, 4, UQ, 4 * T), f32),
        vmem((H, 2, UQ, 4 * T), f32),
        vmem((H, 2, UQ, 4 * T), f32),
        vmem((H, R, hidden), bf16),
        vmem((H, units, 4 * T), f32),
        vmem((H, 2, T, Q), f32),
        vmem((H, 2, T, Q), bf16),
        vmem((H, 2, T, Q), bf16),
        vmem((2, H, T, Q), bf16),
        vmem((2, H, T, Q), bf16),
        dma((3,)),
    ]
    for shape in ((2, H, NC + 1), (2, H, NC + 1), (H, 8), (H, 4), (H, 4), (H, 4), (H, 2), (2, H, NC)):
        scratch += [dma(shape), dma(shape)]
    return pl.pallas_call(
        functools.partial(layer_kernel, (nz, nsub, cap, units)),
        out_shape=jax.ShapeDtypeStruct((T, Q), bf16),
        in_specs=[vspec] * 5 + [hspec] * 3,
        out_specs=vspec,
        scratch_shapes=scratch,
        compiler_params=pltpu.CompilerParams(
            collective_id=0, has_side_effects=True, vmem_limit_bytes=67043328
        ),
    )(
        tokens,
        meta,
        shared_gate,
        shared_up,
        shared_down,
        gate_weight[0],
        up_weight[0],
        down_weight[0],
    )


def solution(mesh):
    in_specs = (
        P(("groups", "ep"), "sub"),
        P(("groups", "ep"), None),
        P(("groups", "ep"), None),
        P("ep", "sub", None),
        P("ep", "sub", None),
        P("ep", None, "sub"),
        P("ep", "sub"),
        P("ep", "sub"),
        P("ep", "sub"),
    )
    out_specs = P(("groups", "ep"), "sub")
    return jax.shard_map(
        per_device, mesh=mesh, in_specs=in_specs, out_specs=out_specs, check_vma=False
    )
```

```python
import functools

import jax
import jax.numpy as jnp
from jax import lax
from jax.experimental import pallas as pl
from jax.experimental.pallas import tpu as pltpu
from jax.sharding import PartitionSpec as P

MESH = pl.DeviceIdType.MESH
NC = 4


def layer_kernel(
    dims,
    ids_ref,
    route_ref,
    tokens_hbm,
    sgate_hbm,
    sup_hbm,
    sdown_hbm,
    gate_hbm,
    up_hbm,
    down_hbm,
    out_ref,
    sgate_ref,
    sup_ref,
    sdown_ref,
    gate_v,
    up_v,
    down_v,
    tok,
    meta,
    comp,
    upper,
    lhs_t,
    wsel,
    xs,
    xr1,
    xc,
    xr2,
    ss,
    sr1,
    sc,
    sr2,
    hid,
    hsb,
    con,
    ps,
    pr,
    rs_s,
    rs_r,
    w_sem,
    ag_ss,
    ag_rs,
    dd_ss,
    dd_rs,
    x1_ss,
    x1_rs,
    x2_ss,
    x2_rs,
    h1_ss,
    h1_rs,
    h2_ss,
    h2_rs,
    pd_ss,
    pd_rs,
    r_ss,
    r_rs,
):
    nz, nsub, cap, units = dims
    f32, bf16 = jnp.float32, jnp.bfloat16
    H = nz // 2
    T, Q = tokens_hbm.shape
    CH = T // NC
    R = 4 * cap
    HQ = gate_v.shape[1] // nsub
    UQ = units // nsub
    TILE = 256
    ntile = Q // TILE

    e = lax.axis_index("ep")
    s = lax.axis_index("sub")
    z = e // 2
    c = e % 2
    z_right = {"ep": ((z + 1) % nz) * 2 + c}
    z_left = {"ep": ((z + nz - 1) % nz) * 2 + c}
    z_next = (z_right, z_left)
    partner = {"ep": z * 2 + (1 - c)}
    xR = (s + 1) % nsub
    xL = (s + nsub - 1) % nsub
    xO = (s + 2) % nsub
    x_right = {"sub": xR}
    x_left = {"sub": xL}

    def remote(src, dst, ssem, rsem, dev):
        return pltpu.make_async_remote_copy(
            src_ref=src, dst_ref=dst, send_sem=ssem, recv_sem=rsem, device_id=dev, device_id_type=MESH
        )

    weights = [
        pltpu.make_async_copy(a, b, w_sem.at[n])
        for n, (a, b) in enumerate(
            (
                (gate_hbm, gate_v),
                (up_hbm, up_v),
                (sgate_hbm, sgate_ref),
                (sup_hbm, sup_ref),
                (sdown_hbm, sdown_ref),
                (down_hbm, down_v),
            )
        )
    ]
    own_tokens = tok.at[H - 1, pl.ds(2 * T, T)]
    own_meta = meta.at[H - 1, 2]
    fetch = pltpu.make_async_copy(tokens_hbm, own_tokens, w_sem.at[6])
    fetch.start()
    own_meta[:, 0:T] = ids_ref[...].astype(f32)
    own_meta[:, T : 2 * T] = route_ref[...]

    barrier = pltpu.get_barrier_semaphore()
    for peer in (z_right, z_left, partner, x_right, x_left):
        pl.semaphore_signal(barrier, inc=1, device_id=peer, device_id_type=MESH)
    pl.semaphore_wait(barrier, 5)
    fetch.wait()

    def mine(m, i):
        return (i < NC // 2 or i == NC) if m == 0 else (NC // 2 <= i < NC)

    def slot_of(m, t):
        return m * (1 - t // H)

    def rows_of(d, rel, i):
        return pl.ds((2 * d + rel) * T + i * CH, CH)

    def ring(m, t, i, first=False):
        d = slot_of(m, t)
        if i == NC:
            src = own_meta if first else meta.at[t - 2, 2 * m]
            dst = meta.at[t - 1, 2 * d]
        else:
            src = own_tokens.at[pl.ds(i * CH, CH)] if first else tok.at[t - 2, rows_of(m, 0, i)]
            dst = tok.at[t - 1, rows_of(d, 0, i)]
        return remote(src, dst, ag_ss.at[m, t - 1, i], ag_rs.at[m, t - 1, i], z_next[m])

    def ring_arrival(m, t, i):
        d = slot_of(m, t)
        dst = meta.at[t - 1, 2 * d] if i == NC else tok.at[t - 1, rows_of(d, 0, i)]
        return remote(dst, dst, ag_ss.at[m, t - 1, i], ag_rs.at[m, t - 1, i], z_next[m])

    def hand(d, t, i, own=False):
        if i == NC:
            src = own_meta if own else meta.at[t - 1, 2 * d]
            dst = meta.at[t - 1, 2 * d + 1]
        else:
            src = own_tokens.at[pl.ds(i * CH, CH)] if own else tok.at[t - 1, rows_of(d, 0, i)]
            dst = tok.at[t - 1, rows_of(d, 1, i)]
        return remote(src, dst, dd_ss.at[d, t - 1, i], dd_rs.at[d, t - 1, i], partner)

    order = [0, NC] + list(range(1, NC))
    for i in order:
        for m in (0, 1):
            if H > 1 or mine(m, i):
                ring(m, 1, i, first=True).start()
    for i in order:
        hand(1, H, i, own=True).start()
    for w in weights:
        w.start()

    row_i = lax.broadcasted_iota(jnp.int32, (4 * T, 4 * T), 0)
    col_i = lax.broadcasted_iota(jnp.int32, (4 * T, 4 * T), 1)
    upper[...] = ((row_i < col_i) & (row_i // T == col_i // T)).astype(f32).astype(bf16)

    def forward(t, i):
        for m in (0, 1):

            @pl.when(t < H)
            def _():
                ring_arrival(m, t, i).wait_recv()
                if mine(m, i):
                    ring(m, t + 1, i).start()
                else:

                    @pl.when(t + 1 < H)
                    def _():
                        ring(m, t + 1, i).start()

                hand(m, t, i).start()

            if mine(m, i):

                @pl.when(t == H)
                def _():
                    ring_arrival(m, t, i).wait_recv()
                    hand(0, t, i).start()

    def stage1a(k):
        for d in (0, 1):
            for i in range(NC + 1):
                hand(d, k, i).wait_recv()
        half = lax.broadcasted_iota(jnp.int32, own_meta.shape, 1) < T
        ids, ws = [], []
        for d in (0, 1):
            m0 = meta[k - 1, 2 * d]
            m1 = meta[k - 1, 2 * d + 1]
            ids.append(jnp.where(half, m0, pltpu.roll(m1, T, 1)))
            ws.append(jnp.where(half, pltpu.roll(m0, T, 1), m1))
        ids = jnp.concatenate(ids, axis=1)
        ws = jnp.concatenate(ws, axis=1)
        hit = ids == e.astype(f32)
        sel = jnp.max(jnp.where(hit, 1.0, 0.0), axis=0, keepdims=True)
        wsel[k - 1] = jnp.broadcast_to(
            jnp.sum(jnp.where(hit, ws, 0.0), axis=0, keepdims=True), (8, 4 * T)
        )
        sel8 = jnp.broadcast_to(sel, (16, 4 * T)).astype(bf16)
        pos = jnp.dot(sel8, upper[...], preferred_element_type=f32)[0:1]
        base = (lax.broadcasted_iota(jnp.int32, (1, 4 * T), 1) // T * cap).astype(f32)
        target = jnp.where(sel > 0.0, pos + base, -1.0)
        place = lax.broadcasted_iota(jnp.int32, (R, 4 * T), 0).astype(f32) == target
        place = jnp.where(place, 1.0, 0.0).astype(bf16)
        lhs_t[k - 1, 0:R, :] = place

        comp[...] = jnp.dot(place, tok[k - 1], preferred_element_type=f32).astype(bf16)

    def x_first(k):
        return (
            remote(xs.at[k - 1, xO, 0], xr1.at[k - 1, 0], x1_ss.at[k - 1, 0], x1_rs.at[k - 1, 0], x_right),
            remote(xs.at[k - 1, xO, 1], xr1.at[k - 1, 2], x1_ss.at[k - 1, 2], x1_rs.at[k - 1, 2], x_left),
            remote(ss.at[k - 1, xO, 0], sr1.at[k - 1, 0], x1_ss.at[k - 1, 4], x1_rs.at[k - 1, 4], x_right),
            remote(ss.at[k - 1, xO, 1], sr1.at[k - 1, 2], x1_ss.at[k - 1, 6], x1_rs.at[k - 1, 6], x_left),
            remote(xs.at[k - 1, xR, 1], xr1.at[k - 1, 1], x1_ss.at[k - 1, 1], x1_rs.at[k - 1, 1], x_right),
            remote(xs.at[k - 1, xL, 0], xr1.at[k - 1, 3], x1_ss.at[k - 1, 3], x1_rs.at[k - 1, 3], x_left),
            remote(ss.at[k - 1, xR, 1], sr1.at[k - 1, 1], x1_ss.at[k - 1, 5], x1_rs.at[k - 1, 5], x_right),
            remote(ss.at[k - 1, xL, 0], sr1.at[k - 1, 3], x1_ss.at[k - 1, 7], x1_rs.at[k - 1, 7], x_left),
        )

    def stage1b(k):
        rows = comp[...]

        ga = jnp.dot(rows, gate_v[...], preferred_element_type=f32).astype(bf16)
        ua = jnp.dot(rows, up_v[...], preferred_element_type=f32).astype(bf16)
        for j in range(nsub):
            xs[k - 1, j, 0] = ga[:, j * HQ : (j + 1) * HQ]
            xs[k - 1, j, 1] = ua[:, j * HQ : (j + 1) * HQ]
        contract = (((1,), (1,)), ((), ()))
        pre = lax.dot_general(sgate_ref[...], tok[k - 1], contract, preferred_element_type=f32)
        lin = lax.dot_general(sup_ref[...], tok[k - 1], contract, preferred_element_type=f32)
        for j in range(nsub):
            ss[k - 1, j, 0] = pre[j * UQ : (j + 1) * UQ]
            ss[k - 1, j, 1] = lin[j * UQ : (j + 1) * UQ]
        for copy in x_first(k):
            copy.start()

    def x_second(k):
        return (
            remote(xc.at[k - 1, 0], xr2.at[k - 1, 0], x2_ss.at[k - 1, 0], x2_rs.at[k - 1, 0], x_right),
            remote(xc.at[k - 1, 1], xr2.at[k - 1, 1], x2_ss.at[k - 1, 1], x2_rs.at[k - 1, 1], x_left),
            remote(sc.at[k - 1, 0], sr2.at[k - 1, 0], x2_ss.at[k - 1, 2], x2_rs.at[k - 1, 2], x_right),
            remote(sc.at[k - 1, 1], sr2.at[k - 1, 1], x2_ss.at[k - 1, 3], x2_rs.at[k - 1, 3], x_left),
        )

    def stage2(k):
        first = x_first(k)
        second = x_second(k)
        for m, toward in ((0, xR), (1, xL)):
            first[m].wait_recv()
            xc[k - 1, m] = (
                xs[k - 1, toward, m].astype(f32) + xr1[k - 1, 2 * m].astype(f32)
            ).astype(bf16)
            second[m].start()
        for m, toward in ((0, xR), (1, xL)):
            first[2 + m].wait_recv()
            sc[k - 1, m] = ss[k - 1, toward, m] + sr1[k - 1, 2 * m]
            second[2 + m].start()

    own_cols = pl.ds(pl.multiple_of(s * HQ, HQ), HQ)
    left_cols = pl.ds(pl.multiple_of(xL * HQ, HQ), HQ)
    right_cols = pl.ds(pl.multiple_of(xR * HQ, HQ), HQ)
    far_cols = pl.ds(pl.multiple_of(xO * HQ, HQ), HQ)
    own_rows = pl.ds(pl.multiple_of(s * UQ, UQ), UQ)
    left_rows = pl.ds(pl.multiple_of(xL * UQ, UQ), UQ)
    right_rows = pl.ds(pl.multiple_of(xR * UQ, UQ), UQ)
    far_rows = pl.ds(pl.multiple_of(xO * UQ, UQ), UQ)

    def h_copy(k, n, cols, rows, dev):
        view = hid.at[k - 1, :, cols]
        small = hsb.at[k - 1, rows, :]
        return (
            remote(view, view, h1_ss.at[k - 1, n], h1_rs.at[k - 1, n], dev),
            remote(small, small, h1_ss.at[k - 1, 2 + n], h1_rs.at[k - 1, 2 + n], dev),
        )

    def stage3(k):
        for copy in x_first(k)[4:]:
            copy.wait_recv()
        for copy in x_second(k):
            copy.wait_recv()
        gate = xs[k - 1, s, 0].astype(f32) + xr1[k - 1, 3].astype(f32) + xr2[k - 1, 0].astype(f32)
        up = xs[k - 1, s, 1].astype(f32) + xr1[k - 1, 1].astype(f32) + xr2[k - 1, 1].astype(f32)
        hid[k - 1, :, own_cols] = (gate / (1.0 + jnp.exp(-gate)) * up).astype(bf16)
        sg = ss[k - 1, s, 0] + sr1[k - 1, 3] + sr2[k - 1, 0]
        su = ss[k - 1, s, 1] + sr1[k - 1, 1] + sr2[k - 1, 1]
        hsb[k - 1, own_rows, :] = sg / (1.0 + jnp.exp(-sg)) * su
        for copy in h_copy(k, 0, own_cols, own_rows, x_right) + h_copy(k, 1, own_cols, own_rows, x_left):
            copy.start()

    def h_far(k, n, cols, rows, dev):
        view = hid.at[k - 1, pl.ds(n * (R // 2), R // 2), cols]
        small = hsb.at[k - 1, rows, pl.ds(n * 2 * T, 2 * T)]
        return (
            remote(view, view, h2_ss.at[k - 1, n], h2_rs.at[k - 1, n], dev),
            remote(small, small, h2_ss.at[k - 1, 2 + n], h2_rs.at[k - 1, 2 + n], dev),
        )

    def stage4(k):
        for n, cols, rows, dev in ((0, left_cols, left_rows, x_right), (1, right_cols, right_rows, x_left)):
            for copy in h_copy(k, n, cols, rows, dev):
                copy.wait_recv()
            for copy in h_far(k, n, cols, rows, dev):
                copy.start()

    def give(k, d):
        return remote(ps.at[k - 1, d], pr.at[k - 1, d], pd_ss.at[k - 1, d], pd_rs.at[k - 1, d], partner)

    def stage5(k):
        for n, dev in ((0, x_right), (1, x_left)):
            for copy in h_far(k, n, far_cols, far_rows, dev):
                copy.wait_recv()
        lhs_t[k - 1, R : R + units, :] = hsb[k - 1].astype(bf16)
        both_t = lhs_t[k - 1]
        weight = jnp.sum(both_t[0:R].astype(f32) * wsel[k - 1, 0:1], axis=1, keepdims=True)
        both = jnp.transpose(both_t.astype(f32)).astype(bf16)
        hidden = hid[k - 1]

        o = jnp.dot(hidden, down_v[...], preferred_element_type=f32)
        o = (o * weight).astype(bf16)
        stacked = jnp.concatenate([o, sdown_ref[...]], axis=0)
        part = jnp.dot(both, stacked, preferred_element_type=f32)
        for d in (0, 1):
            con[k - 1, d] = part[2 * d * T : (2 * d + 1) * T]
            ps[k - 1, d] = part[(2 * d + 1) * T : (2 * d + 2) * T].astype(bf16)
        for d in (0, 1):
            give(k, d).start()

    def during(k, stage):
        @pl.when((k >= 1) & (k <= H))
        def _():
            stage(k)

    def step(t, _):
        forward(t, 0)
        forward(t, NC)

        @pl.when(t == 2)
        def _():
            for w in weights:
                w.wait()

        during(t - 1, stage1a)
        forward(t, 1)
        during(t - 1, stage1b)
        forward(t, 2)
        during(t - 5, stage5)
        forward(t, 3)
        during(t - 4, stage4)
        during(t - 3, stage3)
        during(t - 2, stage2)
        return 0

    lax.fori_loop(1, H + 6, step, 0)

    def rows(i):
        return pl.ds(i * CH, CH)

    def pass_on(m, d, i):
        return remote(
            rs_s.at[m, d - 1, rows(i)],
            rs_r.at[m, d - 1, rows(i)],
            r_ss.at[m, d - 1, i],
            r_rs.at[m, d - 1, i],
            z_next[m],
        )

    def own_sum(d, slot, i):
        return con[d - 1, slot, rows(i), :] + pr[d - 1, slot, rows(i), :].astype(f32)

    give(H, 0).wait_recv()
    for i in range(NC):
        m = 0 if mine(0, i) else 1
        rs_s[m, H - 1, rows(i), :] = own_sum(H, 0, i).astype(bf16)
        pass_on(m, H, i).start()

    def back(d, partly):
        give(d, 0).wait_recv()
        give(d, 1).wait_recv()
        for i in range(NC):
            for m in (0, 1):
                total = own_sum(d, 1 - m, i)
                if not partly or mine(m, i):
                    pass_on(m, d + 1, i).wait_recv()
                    total = total + rs_r[m, d, rows(i), :].astype(f32)
                rs_s[m, d - 1, rows(i), :] = total.astype(bf16)
                pass_on(m, d, i).start()

    if H > 1:
        back(H - 1, True)

    def back_step(n, _):
        back(H - 2 - n, False)
        return 0

    lax.fori_loop(0, H - 2, back_step, 0)
    give(H, 1).wait_recv()
    for i in range(NC):
        total = own_sum(H, 1, i)
        for m in (0, 1):
            pass_on(m, 1, i).wait_recv()
            total = total + rs_r[m, 0, rows(i), :].astype(f32)
        out_ref[rows(i), :] = total.astype(bf16)

    def drain(k, _):
        for i in range(NC + 1):
            for m in (0, 1):
                hand(m, k, i).wait_send()

                @pl.when(k < H)
                def _():
                    ring_arrival(m, k, i).wait_send()

                if mine(m, i):

                    @pl.when(k == H)
                    def _():
                        ring_arrival(m, k, i).wait_send()

        for copy in x_first(k) + x_second(k):
            copy.wait_send()
        for n, dev in ((0, x_right), (1, x_left)):
            for copy in h_copy(k, n, own_cols, own_rows, dev) + h_far(k, n, own_cols, own_rows, dev):
                copy.wait_send()
            give(k, n).wait_send()
        for i in range(NC):
            for m in (0, 1):

                @pl.when(k < H)
                def _():
                    pass_on(m, k, i).wait_send()

                if mine(m, i):

                    @pl.when(k == H)
                    def _():
                        pass_on(m, k, i).wait_send()

        return 0

    lax.fori_loop(1, H + 1, drain, 0)


def per_device(
    tokens,
    expert_ids,
    route_weights,
    gate_weight,
    up_weight,
    down_weight,
    shared_gate,
    shared_up,
    shared_down,
):
    f32, bf16 = jnp.float32, jnp.bfloat16
    nep = lax.axis_size("ep")
    nsub = lax.axis_size("sub")
    nz = nep // 2
    H = nz // 2
    T, Q = tokens.shape
    top = expert_ids.shape[1]
    cap = T * top * 3 // (2 * nep)
    units = shared_gate.shape[0]
    hidden = gate_weight.shape[2]
    HQ, UQ, R = hidden // nsub, units // nsub, 4 * cap
    vmem = pltpu.VMEM
    dma = pltpu.SemaphoreType.DMA
    vspec = pl.BlockSpec(memory_space=pltpu.VMEM)
    hspec = pl.BlockSpec(memory_space=pl.ANY)
    scratch = [vmem((units, Q), bf16)] * 3 + [
        vmem((Q, hidden), bf16),
        vmem((Q, hidden), bf16),
        vmem((hidden, Q), bf16),
        vmem((H, 4 * T, Q), bf16),
        vmem((H, 4, top, 2 * T), f32),
        vmem((R, Q), bf16),
        vmem((4 * T, 4 * T), bf16),
        vmem((H, R + units, 4 * T), bf16),
        vmem((H, 8, 4 * T), f32),
        vmem((H, nsub, 2, R, HQ), bf16),
        vmem((H, 4, R, HQ), bf16),
        vmem((H, 2, R, HQ), bf16),
        vmem((H, 2, R, HQ), bf16),
        vmem((H, nsub, 2, UQ, 4 * T), f32),
        vmem((H, 4, UQ, 4 * T), f32),
        vmem((H, 2, UQ, 4 * T), f32),
        vmem((H, 2, UQ, 4 * T), f32),
        vmem((H, R, hidden), bf16),
        vmem((H, units, 4 * T), f32),
        vmem((H, 2, T, Q), f32),
        vmem((H, 2, T, Q), bf16),
        vmem((H, 2, T, Q), bf16),
        vmem((2, H, T, Q), bf16),
        vmem((2, H, T, Q), bf16),
        dma((7,)),
    ]
    for shape in ((2, H, NC + 1), (2, H, NC + 1), (H, 8), (H, 4), (H, 4), (H, 4), (H, 2), (2, H, NC)):
        scratch += [dma(shape), dma(shape)]
    return pl.pallas_call(
        functools.partial(layer_kernel, (nz, nsub, cap, units)),
        out_shape=jax.ShapeDtypeStruct((T, Q), bf16),
        in_specs=[vspec] * 2 + [hspec] * 7,
        out_specs=vspec,
        scratch_shapes=scratch,
        compiler_params=pltpu.CompilerParams(
            collective_id=0, has_side_effects=True, vmem_limit_bytes=67043328
        ),
    )(
        expert_ids.T,
        route_weights.T,
        tokens,
        shared_gate,
        shared_up,
        shared_down,
        gate_weight[0],
        up_weight[0],
        down_weight[0],
    )


def solution(mesh):
    in_specs = (
        P(("groups", "ep"), "sub"),
        P(("groups", "ep"), None),
        P(("groups", "ep"), None),
        P("ep", "sub", None),
        P("ep", "sub", None),
        P("ep", None, "sub"),
        P("ep", "sub"),
        P("ep", "sub"),
        P("ep", "sub"),
    )
    out_specs = P(("groups", "ep"), "sub")
    return jax.shard_map(
        per_device, mesh=mesh, in_specs=in_specs, out_specs=out_specs, check_vma=False
    )
```

```python
import functools

import jax
import jax.numpy as jnp
from jax import lax
from jax.experimental import pallas as pl
from jax.experimental.pallas import tpu as pltpu
from jax.sharding import PartitionSpec as P

MESH = pl.DeviceIdType.MESH
NC = 4


def layer_kernel(
    dims,
    ids_ref,
    route_ref,
    tokens_hbm,
    sgate_hbm,
    sup_hbm,
    sdown_hbm,
    gate_hbm,
    up_hbm,
    down_hbm,
    out_ref,
    sgate_ref,
    sup_ref,
    sdown_ref,
    gate_v,
    up_v,
    down_v,
    tok,
    meta,
    comp,
    upper,
    lhs_t,
    wsel,
    xs,
    xr1,
    xc,
    xr2,
    ss,
    sr1,
    sc,
    sr2,
    hid,
    hsb,
    con,
    ps,
    pr,
    con_far,
    ps_home,
    pr_home,
    rs_s,
    rs_r,
    fin,
    w_sem,
    ag_ss,
    ag_rs,
    a1_ss,
    own_ss,
    own_rs,
    dd_ss,
    dd_rs,
    x1_ss,
    x1_rs,
    x2_ss,
    x2_rs,
    h1_ss,
    h1_rs,
    h2_ss,
    h2_rs,
    pd_ss,
    pd_rs,
    ph_ss,
    ph_rs,
    r_ss,
    r_rs,
    f_rs,
):
    nz, nsub, cap, units = dims
    f32, bf16 = jnp.float32, jnp.bfloat16
    H = nz // 2
    T, Q = tokens_hbm.shape
    CH = T // NC
    R = 4 * cap
    HQ = gate_v.shape[1] // nsub
    UQ = units // nsub
    TILE = 256
    ntile = Q // TILE

    e = lax.axis_index("ep")
    s = lax.axis_index("sub")
    z = e // 2
    c = e % 2
    ahead = (z + 1 + c * (nz - 2)) % nz
    behind = (z + nz - 1 + c * 2) % nz
    z_next = {"ep": ahead * 2 + c}
    z_prev = {"ep": behind * 2 + c}
    right_first = {"ep": ((z + 1) % nz) * 2}
    left_first = {"ep": ((z + nz - 1) % nz) * 2 + 1}
    partner = {"ep": z * 2 + (1 - c)}
    K = H // 2
    turn = max(H + 1, K + 5)
    xR = (s + 1) % nsub
    xL = (s + nsub - 1) % nsub
    xO = (s + 2) % nsub
    x_right = {"sub": xR}
    x_left = {"sub": xL}

    def remote(src, dst, ssem, rsem, dev):
        return pltpu.make_async_remote_copy(
            src_ref=src, dst_ref=dst, send_sem=ssem, recv_sem=rsem, device_id=dev, device_id_type=MESH
        )

    weights = [
        pltpu.make_async_copy(a, b, w_sem.at[n])
        for n, (a, b) in enumerate(
            (
                (gate_hbm, gate_v),
                (up_hbm, up_v),
                (sgate_hbm, sgate_ref),
                (sup_hbm, sup_ref),
                (sdown_hbm, sdown_ref),
                (down_hbm, down_v),
            )
        )
    ]
    own_tokens = tok.at[c * K + K - 1, pl.ds(3 * T, T)]
    own_meta = meta.at[c * K + K - 1, 3]
    fetch = pltpu.make_async_copy(tokens_hbm, own_tokens, w_sem.at[6])
    fetch.start()
    own_meta[:, 0:T] = ids_ref[...].astype(f32)
    own_meta[:, T : 2 * T] = route_ref[...]

    diag_next = {"ep": ahead * 2 + (1 - c)}
    diag_prev = {"ep": behind * 2 + (1 - c)}
    barrier = pltpu.get_barrier_semaphore()
    for peer in (z_next, z_prev, diag_next, diag_prev, partner, x_right, x_left):
        pl.semaphore_signal(barrier, inc=1, device_id=peer, device_id_type=MESH)
    pl.semaphore_wait(barrier, 7)
    fetch.wait()

    def group_of(r, t):
        return r * K + (t - 1) // 2

    def place_of(t, side):
        return (t - 1) % 2 * 2 + side

    def block(r, t, side, start=0, size=T):
        return tok.at[group_of(r, t), pl.ds(pl.multiple_of(place_of(t, side) * T + start, CH), size)]

    def note(r, t, side):
        return meta.at[group_of(r, t), place_of(t, side)]

    half_rows = T // 2

    def send_first(r):
        for m, dev in ((0, right_first), (1, left_first)):
            for i in range(NC + 1):
                src = own_meta if i == NC else own_tokens.at[pl.ds(i * CH, CH)]
                dst = note(r, 1, 0) if i == NC else block(r, 1, 0, i * CH, CH)
                remote(src, dst, a1_ss.at[m, i], ag_rs.at[r, 0, i], dev).start()

    def first_sent(m, i):
        src = own_meta if i == NC else own_tokens.at[pl.ds(i * CH, CH)]
        return remote(src, src, a1_ss.at[m, i], ag_rs.at[0, 0, i], z_next)

    def ring(r, t, i):
        if isinstance(i, int) and i == NC:
            src, dst = note(r, t - 1, 0), note(r, t, 0)
        else:
            src, dst = block(r, t - 1, 0, i * CH, CH), block(r, t, 0, i * CH, CH)
        return remote(src, dst, ag_ss.at[r, t - 1, i], ag_rs.at[r, t - 1, i], z_next)

    def arrival(r, t, i):
        dst = note(r, t, 0) if isinstance(i, int) and i == NC else block(r, t, 0, i * CH, CH)
        return remote(dst, dst, ag_ss.at[r, t - 1, i], ag_rs.at[r, t - 1, i], z_next)

    def hand(r, t):
        return (
            remote(block(r, t, 0), block(r, t, 1), dd_ss.at[r, t - 1, 0], dd_rs.at[r, t - 1, 0], partner),
            remote(note(r, t, 0), note(r, t, 1), dd_ss.at[r, t - 1, 1], dd_rs.at[r, t - 1, 1], partner),
        )

    def hand_far(r, mine):
        view = block(r, H, 0, mine * half_rows, half_rows)
        return remote(view, view, dd_ss.at[r, H - 1, 0], dd_rs.at[r, H - 1, 0], partner)

    def hand_own(r):
        return (
            remote(own_tokens, block(r, H, 1), own_ss.at[0], own_rs.at[0], partner),
            remote(own_meta, note(r, H, 1), own_ss.at[1], own_rs.at[1], partner),
        )

    def own_arrival(r):
        return (
            remote(block(r, H, 1), block(r, H, 1), own_ss.at[0], own_rs.at[0], partner),
            remote(note(r, H, 1), note(r, H, 1), own_ss.at[1], own_rs.at[1], partner),
        )

    @pl.when(c == 0)
    def _():
        send_first(0)

    for copy in hand_own(c):
        copy.start()
    for w in weights:
        w.start()

    row_i = lax.broadcasted_iota(jnp.int32, (4 * T, 4 * T), 0)
    col_i = lax.broadcasted_iota(jnp.int32, (4 * T, 4 * T), 1)
    upper[...] = ((row_i < col_i) & (row_i // T == col_i // T)).astype(f32).astype(bf16)

    def forward(p, sub, i):
        r = (p - 1) // K
        kk = (p - 1) % K + 1
        t = 2 * kk - 1 + sub
        last = kk == K

        @pl.when(p <= H)
        def _():
            if i == NC:
                arrival(r, t, i).wait_recv()
                if sub == 0:
                    ring(r, t + 1, i).start()
                else:

                    @pl.when(kk < K)
                    def _():
                        ring(r, t + 1, i).start()

            elif sub == 0:
                arrival(r, t, i).wait_recv()

                @pl.when((kk < K) | (c == i // (NC // 2)))
                def _():
                    ring(r, t + 1, i).start()

            else:

                @pl.when((kk < K) | (c == i // (NC // 2)))
                def _():
                    arrival(r, t, i).wait_recv()

                @pl.when(kk < K)
                def _():
                    ring(r, t + 1, i).start()

            if i == NC - 1:
                if sub == 0:
                    for copy in hand(r, t):
                        copy.start()
                else:

                    @pl.when(kk < K)
                    def _():
                        for copy in hand(r, t):
                            copy.start()

                    @pl.when(last)
                    def _():
                        hand_far(r, c).start()

    def stage1a(k):
        r = (k - 1) // K
        kk = (k - 1) % K + 1
        for copy in hand(r, 2 * kk - 1):
            copy.wait_recv()

        @pl.when(kk < K)
        def _():
            for copy in hand(r, 2 * kk):
                copy.wait_recv()

        @pl.when(kk == K)
        def _():
            hand_far(r, 1 - c).wait_recv()

            @pl.when(c != r)
            def _():
                for copy in own_arrival(r):
                    copy.wait_recv()

        half = lax.broadcasted_iota(jnp.int32, own_meta.shape, 1) < T
        ids, ws = [], []
        for d in (0, 1):
            m0 = meta[k - 1, 2 * d]
            m1 = meta[k - 1, 2 * d + 1]
            ids.append(jnp.where(half, m0, pltpu.roll(m1, T, 1)))
            ws.append(jnp.where(half, pltpu.roll(m0, T, 1), m1))
        ids = jnp.concatenate(ids, axis=1)
        ws = jnp.concatenate(ws, axis=1)
        hit = ids == e.astype(f32)
        sel = jnp.max(jnp.where(hit, 1.0, 0.0), axis=0, keepdims=True)
        wsel[k - 1] = jnp.broadcast_to(
            jnp.sum(jnp.where(hit, ws, 0.0), axis=0, keepdims=True), (8, 4 * T)
        )
        sel8 = jnp.broadcast_to(sel, (16, 4 * T)).astype(bf16)
        pos = jnp.dot(sel8, upper[...], preferred_element_type=f32)[0:1]
        base = (lax.broadcasted_iota(jnp.int32, (1, 4 * T), 1) // T * cap).astype(f32)
        target = jnp.where(sel > 0.0, pos + base, -1.0)
        place = lax.broadcasted_iota(jnp.int32, (R, 4 * T), 0).astype(f32) == target
        place = jnp.where(place, 1.0, 0.0).astype(bf16)
        lhs_t[k - 1, 0:R, :] = place

        comp[...] = jnp.dot(place, tok[k - 1], preferred_element_type=f32).astype(bf16)

    def x_first(k):
        return (
            remote(xs.at[k - 1, xO, 0], xr1.at[k - 1, 0], x1_ss.at[k - 1, 0], x1_rs.at[k - 1, 0], x_right),
            remote(xs.at[k - 1, xO, 1], xr1.at[k - 1, 2], x1_ss.at[k - 1, 2], x1_rs.at[k - 1, 2], x_left),
            remote(ss.at[k - 1, xO, 0], sr1.at[k - 1, 0], x1_ss.at[k - 1, 4], x1_rs.at[k - 1, 4], x_right),
            remote(ss.at[k - 1, xO, 1], sr1.at[k - 1, 2], x1_ss.at[k - 1, 6], x1_rs.at[k - 1, 6], x_left),
            remote(xs.at[k - 1, xR, 1], xr1.at[k - 1, 1], x1_ss.at[k - 1, 1], x1_rs.at[k - 1, 1], x_right),
            remote(xs.at[k - 1, xL, 0], xr1.at[k - 1, 3], x1_ss.at[k - 1, 3], x1_rs.at[k - 1, 3], x_left),
            remote(ss.at[k - 1, xR, 1], sr1.at[k - 1, 1], x1_ss.at[k - 1, 5], x1_rs.at[k - 1, 5], x_right),
            remote(ss.at[k - 1, xL, 0], sr1.at[k - 1, 3], x1_ss.at[k - 1, 7], x1_rs.at[k - 1, 7], x_left),
        )

    def stage1b(k):
        rows = comp[...]

        ga = jnp.dot(rows, gate_v[...], preferred_element_type=f32).astype(bf16)
        ua = jnp.dot(rows, up_v[...], preferred_element_type=f32).astype(bf16)
        for j in range(nsub):
            xs[k - 1, j, 0] = ga[:, j * HQ : (j + 1) * HQ]
            xs[k - 1, j, 1] = ua[:, j * HQ : (j + 1) * HQ]
        contract = (((1,), (1,)), ((), ()))
        pre = lax.dot_general(sgate_ref[...], tok[k - 1], contract, preferred_element_type=f32)
        lin = lax.dot_general(sup_ref[...], tok[k - 1], contract, preferred_element_type=f32)
        for j in range(nsub):
            ss[k - 1, j, 0] = pre[j * UQ : (j + 1) * UQ]
            ss[k - 1, j, 1] = lin[j * UQ : (j + 1) * UQ]
        for copy in x_first(k):
            copy.start()

    def x_second(k):
        return (
            remote(xc.at[k - 1, 0], xr2.at[k - 1, 0], x2_ss.at[k - 1, 0], x2_rs.at[k - 1, 0], x_right),
            remote(xc.at[k - 1, 1], xr2.at[k - 1, 1], x2_ss.at[k - 1, 1], x2_rs.at[k - 1, 1], x_left),
            remote(sc.at[k - 1, 0], sr2.at[k - 1, 0], x2_ss.at[k - 1, 2], x2_rs.at[k - 1, 2], x_right),
            remote(sc.at[k - 1, 1], sr2.at[k - 1, 1], x2_ss.at[k - 1, 3], x2_rs.at[k - 1, 3], x_left),
        )

    def stage2(k):
        first = x_first(k)
        second = x_second(k)
        for m, toward in ((0, xR), (1, xL)):
            first[m].wait_recv()
            xc[k - 1, m] = (
                xs[k - 1, toward, m].astype(f32) + xr1[k - 1, 2 * m].astype(f32)
            ).astype(bf16)
            second[m].start()
        for m, toward in ((0, xR), (1, xL)):
            first[2 + m].wait_recv()
            sc[k - 1, m] = ss[k - 1, toward, m] + sr1[k - 1, 2 * m]
            second[2 + m].start()

    own_cols = pl.ds(pl.multiple_of(s * HQ, HQ), HQ)
    left_cols = pl.ds(pl.multiple_of(xL * HQ, HQ), HQ)
    right_cols = pl.ds(pl.multiple_of(xR * HQ, HQ), HQ)
    far_cols = pl.ds(pl.multiple_of(xO * HQ, HQ), HQ)
    own_rows = pl.ds(pl.multiple_of(s * UQ, UQ), UQ)
    left_rows = pl.ds(pl.multiple_of(xL * UQ, UQ), UQ)
    right_rows = pl.ds(pl.multiple_of(xR * UQ, UQ), UQ)
    far_rows = pl.ds(pl.multiple_of(xO * UQ, UQ), UQ)

    def h_copy(k, n, cols, rows, dev):
        view = hid.at[k - 1, :, cols]
        small = hsb.at[k - 1, rows, :]
        return (
            remote(view, view, h1_ss.at[k - 1, n], h1_rs.at[k - 1, n], dev),
            remote(small, small, h1_ss.at[k - 1, 2 + n], h1_rs.at[k - 1, 2 + n], dev),
        )

    def stage3(k):
        for copy in x_first(k)[4:]:
            copy.wait_recv()
        for copy in x_second(k):
            copy.wait_recv()
        gate = xs[k - 1, s, 0].astype(f32) + xr1[k - 1, 3].astype(f32) + xr2[k - 1, 0].astype(f32)
        up = xs[k - 1, s, 1].astype(f32) + xr1[k - 1, 1].astype(f32) + xr2[k - 1, 1].astype(f32)
        hid[k - 1, :, own_cols] = (gate / (1.0 + jnp.exp(-gate)) * up).astype(bf16)
        sg = ss[k - 1, s, 0] + sr1[k - 1, 3] + sr2[k - 1, 0]
        su = ss[k - 1, s, 1] + sr1[k - 1, 1] + sr2[k - 1, 1]
        hsb[k - 1, own_rows, :] = sg / (1.0 + jnp.exp(-sg)) * su
        for copy in h_copy(k, 0, own_cols, own_rows, x_right) + h_copy(k, 1, own_cols, own_rows, x_left):
            copy.start()

    def h_far(k, n, cols, rows, dev):
        view = hid.at[k - 1, pl.ds(n * (R // 2), R // 2), cols]
        small = hsb.at[k - 1, rows, pl.ds(n * 2 * T, 2 * T)]
        return (
            remote(view, view, h2_ss.at[k - 1, n], h2_rs.at[k - 1, n], dev),
            remote(small, small, h2_ss.at[k - 1, 2 + n], h2_rs.at[k - 1, 2 + n], dev),
        )

    def stage4(k):
        for n, cols, rows, dev in ((0, left_cols, left_rows, x_right), (1, right_cols, right_rows, x_left)):
            for copy in h_copy(k, n, cols, rows, dev):
                copy.wait_recv()
            for copy in h_far(k, n, cols, rows, dev):
                copy.start()

    def give(r, k):
        return remote(ps.at[r, k - 1], pr.at[r, k - 1], pd_ss.at[r, k - 1], pd_rs.at[r, k - 1], partner)

    def give_far(r, theirs):
        rows = pl.ds(pl.multiple_of(theirs * half_rows, CH), half_rows)
        return remote(
            ps.at[r, H - 1, rows], pr.at[r, H - 1, rows], pd_ss.at[r, H - 1], pd_rs.at[r, H - 1], partner
        )

    def give_home(r):
        return remote(ps_home.at[r], pr_home.at[r], ph_ss.at[r], ph_rs.at[r], partner)

    def stage5(k):
        for n, dev in ((0, x_right), (1, x_left)):
            for copy in h_far(k, n, far_cols, far_rows, dev):
                copy.wait_recv()
        lhs_t[k - 1, R : R + units, :] = hsb[k - 1].astype(bf16)
        both_t = lhs_t[k - 1]
        weight = jnp.sum(both_t[0:R].astype(f32) * wsel[k - 1, 0:1], axis=1, keepdims=True)
        both = jnp.transpose(both_t.astype(f32)).astype(bf16)
        hidden = hid[k - 1]

        o = jnp.dot(hidden, down_v[...], preferred_element_type=f32)
        o = (o * weight).astype(bf16)
        stacked = jnp.concatenate([o, sdown_ref[...]], axis=0)
        part = jnp.dot(both, stacked, preferred_element_type=f32)
        r = (k - 1) // K
        kk = (k - 1) % K + 1
        for n in (0, 1):
            ps[r, 2 * kk - 2 + n] = part[2 * n * T : (2 * n + 1) * T].astype(bf16)
            con[r, 2 * kk - 2 + n] = part[(2 * n + 1) * T : (2 * n + 2) * T]
        give(r, 2 * kk - 1).start()

        @pl.when(kk < K)
        def _():
            give(r, 2 * kk).start()

        @pl.when(kk == K)
        def _():
            con_far[r] = part[2 * T : 3 * T]
            ps_home[r] = part[3 * T : 4 * T].astype(bf16)
            give_far(r, 1 - c).start()
            give_home(r).start()

    def during(k, stage):
        @pl.when((k >= 1) & (k <= H))
        def _():
            stage(k)

    def step(p, _):
        @pl.when((p == K) & (c == 1))
        def _():
            send_first(1)

        forward(p, 0, 0)
        forward(p, 0, NC)
        forward(p, 0, 1)

        @pl.when(p == 2)
        def _():
            for w in weights:
                w.wait()

        during(p - 1, stage1a)
        forward(p, 0, 2)
        forward(p, 0, 3)
        during(p - 1, stage1b)
        forward(p, 1, 0)
        forward(p, 1, NC)
        forward(p, 1, 1)
        during(p - 5, stage5)
        forward(p, 1, 2)
        forward(p, 1, 3)

        @pl.when(p >= turn)
        def _():
            d = H + turn - p

            @pl.when(d >= 1)
            def _():
                back(0, d)

        during(p - 4, stage4)
        during(p - 3, stage3)
        during(p - 2, stage2)
        return 0

    def rows(i):
        return pl.ds(pl.multiple_of(i * CH, CH), CH)

    def pass_on(r, d, i):
        return remote(
            rs_s.at[r, d - 1, rows(i)],
            rs_r.at[r, d - 1, rows(i)],
            r_ss.at[r, d - 1, i],
            r_rs.at[r, d - 1, i],
            z_next,
        )

    def pass_home(r, i):
        return remote(
            rs_s.at[r, 0, rows(i)],
            fin.at[c, rows(i)],
            r_ss.at[r, 0, i],
            f_rs.at[c, i],
            {"ep": ahead * 2 + r},
        )

    def own_sum(r, d, i):
        return con[r, d - 1, rows(i), :] + pr[r, d - 1, rows(i), :].astype(f32)

    def emit(r, d, i, total):
        rs_s[r, d - 1, rows(i), :] = total.astype(bf16)

        @pl.when(d > 1)
        def _():
            pass_on(r, d, i).start()

        @pl.when(d == 1)
        def _():
            pass_home(r, i).start()

    def back(r, d):
        @pl.when(d == H)
        def _():
            give_far(r, c).wait_recv()
            for j in range(NC // 2):
                i = c * (NC // 2) + j
                total = con_far[r, rows(i), :] + pr[r, H - 1, rows(i), :].astype(f32)
                emit(r, d, i, total)

        @pl.when(d < H)
        def _():
            give(r, d).wait_recv()

        @pl.when(d == H - 1)
        def _():
            for j in range(NC // 2):
                i = (1 - c) * (NC // 2) + j
                emit(r, d, i, own_sum(r, d, i))
            for j in range(NC // 2):
                i = c * (NC // 2) + j
                pass_on(r, d + 1, i).wait_recv()
                emit(r, d, i, own_sum(r, d, i) + rs_r[r, d, rows(i), :].astype(f32))

        @pl.when(d < H - 1)
        def _():
            for i in range(NC):
                pass_on(r, d + 1, i).wait_recv()
                emit(r, d, i, own_sum(r, d, i) + rs_r[r, d, rows(i), :].astype(f32))

    lax.fori_loop(1, H + 6, step, 0)

    def rest(n, _):
        left = turn - 6
        r = jnp.where(n < left, 0, 1)
        d = jnp.where(n < left, left - n, H + left - n)
        back(r, d)
        return 0

    lax.fori_loop(0, turn - 6 + H, rest, 0)
    for r in (0, 1):
        give_home(r).wait_recv()
    for i in range(NC):
        total = con[c, H - 1, rows(i), :] + pr_home[c, rows(i), :].astype(f32)
        for m in (0, 1):
            remote(fin.at[m, rows(i)], fin.at[m, rows(i)], r_ss.at[0, 0, i], f_rs.at[m, i], z_next).wait_recv()
            total = total + fin[m, rows(i), :].astype(f32)
        out_ref[rows(i), :] = total.astype(bf16)

    for i in range(NC + 1):
        for m in (0, 1):
            first_sent(m, i).wait_send()
    for copy in hand_own(c):
        copy.wait_send()

    def drain(k, _):
        for r in (0, 1):

            @pl.when(k < H)
            def _():
                for copy in hand(r, k):
                    copy.wait_send()
                give(r, k).wait_send()
                for i in range(NC):
                    pass_on(r, k, i).wait_send()

            @pl.when((k > 1) & (k < H))
            def _():
                for i in range(NC):
                    arrival(r, k, i).wait_send()

            @pl.when(k > 1)
            def _():
                arrival(r, k, NC).wait_send()

            @pl.when(k == H)
            def _():
                hand_far(r, c).wait_send()
                give_far(r, 1 - c).wait_send()
                give_home(r).wait_send()
                for j in range(NC // 2):
                    i = c * (NC // 2) + j
                    arrival(r, k, i).wait_send()
                    pass_on(r, k, i).wait_send()

        for copy in x_first(k) + x_second(k):
            copy.wait_send()
        for n, dev in ((0, x_right), (1, x_left)):
            for copy in h_copy(k, n, own_cols, own_rows, dev) + h_far(k, n, own_cols, own_rows, dev):
                copy.wait_send()
        return 0

    lax.fori_loop(1, H + 1, drain, 0)


def per_device(
    tokens,
    expert_ids,
    route_weights,
    gate_weight,
    up_weight,
    down_weight,
    shared_gate,
    shared_up,
    shared_down,
):
    f32, bf16 = jnp.float32, jnp.bfloat16
    nep = lax.axis_size("ep")
    nsub = lax.axis_size("sub")
    nz = nep // 2
    H = nz // 2
    T, Q = tokens.shape
    top = expert_ids.shape[1]
    cap = T * top * 3 // (2 * nep)
    units = shared_gate.shape[0]
    hidden = gate_weight.shape[2]
    HQ, UQ, R = hidden // nsub, units // nsub, 4 * cap
    vmem = pltpu.VMEM
    dma = pltpu.SemaphoreType.DMA
    vspec = pl.BlockSpec(memory_space=pltpu.VMEM)
    hspec = pl.BlockSpec(memory_space=pl.ANY)
    scratch = [vmem((units, Q), bf16)] * 3 + [
        vmem((Q, hidden), bf16),
        vmem((Q, hidden), bf16),
        vmem((hidden, Q), bf16),
        vmem((H, 4 * T, Q), bf16),
        vmem((H, 4, top, 2 * T), f32),
        vmem((R, Q), bf16),
        vmem((4 * T, 4 * T), bf16),
        vmem((H, R + units, 4 * T), bf16),
        vmem((H, 8, 4 * T), f32),
        vmem((H, nsub, 2, R, HQ), bf16),
        vmem((H, 4, R, HQ), bf16),
        vmem((H, 2, R, HQ), bf16),
        vmem((H, 2, R, HQ), bf16),
        vmem((H, nsub, 2, UQ, 4 * T), f32),
        vmem((H, 4, UQ, 4 * T), f32),
        vmem((H, 2, UQ, 4 * T), f32),
        vmem((H, 2, UQ, 4 * T), f32),
        vmem((H, R, hidden), bf16),
        vmem((H, units, 4 * T), f32),
        vmem((2, H, T, Q), f32),
        vmem((2, H, T, Q), bf16),
        vmem((2, H, T, Q), bf16),
        vmem((2, T, Q), f32),
        vmem((2, T, Q), bf16),
        vmem((2, T, Q), bf16),
        vmem((2, H, T, Q), bf16),
        vmem((2, H, T, Q), bf16),
        vmem((2, T, Q), bf16),
        dma((7,)),
    ]
    scratch += [dma((2, H, NC + 1)), dma((2, H, NC + 1)), dma((2, NC + 1))]
    for shape in ((2,), (2, H, 2), (H, 8), (H, 4), (H, 4), (H, 4), (2, H), (2,), (2, H, NC)):
        scratch += [dma(shape), dma(shape)]
    scratch.append(dma((2, NC)))
    return pl.pallas_call(
        functools.partial(layer_kernel, (nz, nsub, cap, units)),
        out_shape=jax.ShapeDtypeStruct((T, Q), bf16),
        in_specs=[vspec] * 2 + [hspec] * 7,
        out_specs=vspec,
        scratch_shapes=scratch,
        compiler_params=pltpu.CompilerParams(
            collective_id=0, has_side_effects=True, vmem_limit_bytes=67043328
        ),
    )(
        expert_ids.T,
        route_weights.T,
        tokens,
        shared_gate,
        shared_up,
        shared_down,
        gate_weight[0],
        up_weight[0],
        down_weight[0],
    )


def solution(mesh):
    in_specs = (
        P(("groups", "ep"), "sub"),
        P(("groups", "ep"), None),
        P(("groups", "ep"), None),
        P("ep", "sub", None),
        P("ep", "sub", None),
        P("ep", None, "sub"),
        P("ep", "sub"),
        P("ep", "sub"),
        P("ep", "sub"),
    )
    out_specs = P(("groups", "ep"), "sub")
    return jax.shard_map(
        per_device, mesh=mesh, in_specs=in_specs, out_specs=out_specs, check_vma=False
    )
```

```python
import functools

import jax
import jax.numpy as jnp
from jax import lax
from jax.experimental import pallas as pl
from jax.experimental.pallas import tpu as pltpu
from jax.sharding import PartitionSpec as P

MESH = pl.DeviceIdType.MESH
NC = 4


def layer_kernel(
    dims,
    ids_ref,
    route_ref,
    tokens_hbm,
    sgate_hbm,
    sup_hbm,
    sdown_hbm,
    gate_hbm,
    up_hbm,
    down_hbm,
    out_ref,
    sgate_ref,
    sup_ref,
    sdown_ref,
    gate_v,
    up_v,
    down_v,
    tok,
    meta,
    comp,
    upper,
    lhs_t,
    wsel,
    xs,
    xr1,
    xc,
    xr2,
    ss,
    sr1,
    sc,
    sr2,
    hid,
    hsb,
    con,
    ps,
    pr,
    rs_s,
    rs_r,
    w_sem,
    ag_ss,
    ag_rs,
    dd_ss,
    dd_rs,
    x1_ss,
    x1_rs,
    x2_ss,
    x2_rs,
    h1_ss,
    h1_rs,
    h2_ss,
    h2_rs,
    pd_ss,
    pd_rs,
    r_ss,
    r_rs,
):
    nz, nsub, cap, units = dims
    f32, bf16 = jnp.float32, jnp.bfloat16
    H = nz // 2
    T, Q = tokens_hbm.shape
    CH = T // NC
    R = 4 * cap
    HQ = gate_v.shape[1] // nsub
    UQ = units // nsub
    TILE = 256
    ntile = Q // TILE

    e = lax.axis_index("ep")
    s = lax.axis_index("sub")
    z = e // 2
    c = e % 2
    z_right = {"ep": ((z + 1) % nz) * 2 + c}
    z_left = {"ep": ((z + nz - 1) % nz) * 2 + c}
    z_next = (z_right, z_left)
    partner = {"ep": z * 2 + (1 - c)}
    xR = (s + 1) % nsub
    xL = (s + nsub - 1) % nsub
    xO = (s + 2) % nsub
    x_right = {"sub": xR}
    x_left = {"sub": xL}

    def remote(src, dst, ssem, rsem, dev):
        return pltpu.make_async_remote_copy(
            src_ref=src, dst_ref=dst, send_sem=ssem, recv_sem=rsem, device_id=dev, device_id_type=MESH
        )

    weights = [
        pltpu.make_async_copy(a, b, w_sem.at[n])
        for n, (a, b) in enumerate(
            (
                (gate_hbm, gate_v),
                (up_hbm, up_v),
                (sgate_hbm, sgate_ref),
                (sup_hbm, sup_ref),
                (sdown_hbm, sdown_ref),
                (down_hbm, down_v),
            )
        )
    ]
    own_tokens = tok.at[H - 1, pl.ds(2 * T, T)]
    own_meta = meta.at[H - 1, 2]
    fetch = pltpu.make_async_copy(tokens_hbm, own_tokens, w_sem.at[6])
    fetch.start()
    own_meta[:, 0:T] = ids_ref[...].astype(f32)
    own_meta[:, T : 2 * T] = route_ref[...]

    barrier = pltpu.get_barrier_semaphore()
    for peer in (z_right, z_left, partner, x_right, x_left):
        pl.semaphore_signal(barrier, inc=1, device_id=peer, device_id_type=MESH)
    pl.semaphore_wait(barrier, 5)
    fetch.wait()

    def mine(m, i):
        return (i < NC // 2 or i == NC) if m == 0 else (NC // 2 <= i < NC)

    def slot_of(m, t):
        return m * (1 - t // H)

    def rows_of(d, rel, i):
        return pl.ds((2 * d + rel) * T + i * CH, CH)

    def ring(m, t, i, first=False):
        d = slot_of(m, t)
        if i == NC:
            src = own_meta if first else meta.at[t - 2, 2 * m]
            dst = meta.at[t - 1, 2 * d]
        else:
            src = own_tokens.at[pl.ds(i * CH, CH)] if first else tok.at[t - 2, rows_of(m, 0, i)]
            dst = tok.at[t - 1, rows_of(d, 0, i)]
        return remote(src, dst, ag_ss.at[m, t - 1, i], ag_rs.at[m, t - 1, i], z_next[m])

    def ring_arrival(m, t, i):
        d = slot_of(m, t)
        dst = meta.at[t - 1, 2 * d] if i == NC else tok.at[t - 1, rows_of(d, 0, i)]
        return remote(dst, dst, ag_ss.at[m, t - 1, i], ag_rs.at[m, t - 1, i], z_next[m])

    def hand(d, t, i, own=False):
        if i == NC:
            src = own_meta if own else meta.at[t - 1, 2 * d]
            dst = meta.at[t - 1, 2 * d + 1]
        else:
            src = own_tokens.at[pl.ds(i * CH, CH)] if own else tok.at[t - 1, rows_of(d, 0, i)]
            dst = tok.at[t - 1, rows_of(d, 1, i)]
        return remote(src, dst, dd_ss.at[d, t - 1, i], dd_rs.at[d, t - 1, i], partner)

    order = [0, NC] + list(range(1, NC))
    for i in order:
        for m in (0, 1):
            if H > 1 or mine(m, i):
                ring(m, 1, i, first=True).start()
    for i in order:
        hand(1, H, i, own=True).start()
    for w in weights:
        w.start()

    row_i = lax.broadcasted_iota(jnp.int32, (4 * T, 4 * T), 0)
    col_i = lax.broadcasted_iota(jnp.int32, (4 * T, 4 * T), 1)
    upper[...] = ((row_i < col_i) & (row_i // T == col_i // T)).astype(f32).astype(bf16)

    def forward(t, i):
        for m in (0, 1):

            @pl.when(t < H)
            def _():
                ring_arrival(m, t, i).wait_recv()
                if mine(m, i):
                    ring(m, t + 1, i).start()
                else:

                    @pl.when(t + 1 < H)
                    def _():
                        ring(m, t + 1, i).start()

                hand(m, t, i).start()

            if mine(m, i):

                @pl.when(t == H)
                def _():
                    ring_arrival(m, t, i).wait_recv()
                    hand(0, t, i).start()

    def stage1a(k):
        for d in (0, 1):
            for i in range(NC + 1):
                hand(d, k, i).wait_recv()
        half = lax.broadcasted_iota(jnp.int32, own_meta.shape, 1) < T
        ids, ws = [], []
        for d in (0, 1):
            m0 = meta[k - 1, 2 * d]
            m1 = meta[k - 1, 2 * d + 1]
            ids.append(jnp.where(half, m0, pltpu.roll(m1, T, 1)))
            ws.append(jnp.where(half, pltpu.roll(m0, T, 1), m1))
        ids = jnp.concatenate(ids, axis=1)
        ws = jnp.concatenate(ws, axis=1)
        hit = ids == e.astype(f32)
        sel = jnp.max(jnp.where(hit, 1.0, 0.0), axis=0, keepdims=True)
        wsel[k - 1] = jnp.broadcast_to(
            jnp.sum(jnp.where(hit, ws, 0.0), axis=0, keepdims=True), (8, 4 * T)
        )
        sel8 = jnp.broadcast_to(sel, (16, 4 * T)).astype(bf16)
        pos = jnp.dot(sel8, upper[...], preferred_element_type=f32)[0:1]
        base = (lax.broadcasted_iota(jnp.int32, (1, 4 * T), 1) // T * cap).astype(f32)
        target = jnp.where(sel > 0.0, pos + base, -1.0)
        place = lax.broadcasted_iota(jnp.int32, (R, 4 * T), 0).astype(f32) == target
        place = jnp.where(place, 1.0, 0.0).astype(bf16)
        lhs_t[k - 1, 0:R, :] = place

        comp[...] = jnp.dot(place, tok[k - 1], preferred_element_type=f32).astype(bf16)

    def x_first(k):
        return (
            remote(xs.at[k - 1, xO, 0], xr1.at[k - 1, 0], x1_ss.at[k - 1, 0], x1_rs.at[k - 1, 0], x_right),
            remote(xs.at[k - 1, xO, 1], xr1.at[k - 1, 2], x1_ss.at[k - 1, 2], x1_rs.at[k - 1, 2], x_left),
            remote(ss.at[k - 1, xO, 0], sr1.at[k - 1, 0], x1_ss.at[k - 1, 4], x1_rs.at[k - 1, 4], x_right),
            remote(ss.at[k - 1, xO, 1], sr1.at[k - 1, 2], x1_ss.at[k - 1, 6], x1_rs.at[k - 1, 6], x_left),
            remote(xs.at[k - 1, xR, 1], xr1.at[k - 1, 1], x1_ss.at[k - 1, 1], x1_rs.at[k - 1, 1], x_right),
            remote(xs.at[k - 1, xL, 0], xr1.at[k - 1, 3], x1_ss.at[k - 1, 3], x1_rs.at[k - 1, 3], x_left),
            remote(ss.at[k - 1, xR, 1], sr1.at[k - 1, 1], x1_ss.at[k - 1, 5], x1_rs.at[k - 1, 5], x_right),
            remote(ss.at[k - 1, xL, 0], sr1.at[k - 1, 3], x1_ss.at[k - 1, 7], x1_rs.at[k - 1, 7], x_left),
        )

    def stage1b(k):
        rows = comp[...]

        first = x_first(k)
        ga = jnp.dot(rows, gate_v[...], preferred_element_type=f32).astype(bf16)
        for j in range(nsub):
            xs[k - 1, j, 0] = ga[:, j * HQ : (j + 1) * HQ]
        first[0].start()
        ua = jnp.dot(rows, up_v[...], preferred_element_type=f32).astype(bf16)
        for j in range(nsub):
            xs[k - 1, j, 1] = ua[:, j * HQ : (j + 1) * HQ]
        first[1].start()
        contract = (((1,), (1,)), ((), ()))
        pre = lax.dot_general(sgate_ref[...], tok[k - 1], contract, preferred_element_type=f32)
        lin = lax.dot_general(sup_ref[...], tok[k - 1], contract, preferred_element_type=f32)
        for j in range(nsub):
            ss[k - 1, j, 0] = pre[j * UQ : (j + 1) * UQ]
            ss[k - 1, j, 1] = lin[j * UQ : (j + 1) * UQ]
        for copy in first[2:]:
            copy.start()

    def x_second(k):
        return (
            remote(xc.at[k - 1, 0], xr2.at[k - 1, 0], x2_ss.at[k - 1, 0], x2_rs.at[k - 1, 0], x_right),
            remote(xc.at[k - 1, 1], xr2.at[k - 1, 1], x2_ss.at[k - 1, 1], x2_rs.at[k - 1, 1], x_left),
            remote(sc.at[k - 1, 0], sr2.at[k - 1, 0], x2_ss.at[k - 1, 2], x2_rs.at[k - 1, 2], x_right),
            remote(sc.at[k - 1, 1], sr2.at[k - 1, 1], x2_ss.at[k - 1, 3], x2_rs.at[k - 1, 3], x_left),
        )

    def stage2(k):
        first = x_first(k)
        second = x_second(k)
        for m, toward in ((0, xR), (1, xL)):
            first[m].wait_recv()
            xc[k - 1, m] = (
                xs[k - 1, toward, m].astype(f32) + xr1[k - 1, 2 * m].astype(f32)
            ).astype(bf16)
            second[m].start()
        for m, toward in ((0, xR), (1, xL)):
            first[2 + m].wait_recv()
            sc[k - 1, m] = ss[k - 1, toward, m] + sr1[k - 1, 2 * m]
            second[2 + m].start()

    own_cols = pl.ds(pl.multiple_of(s * HQ, HQ), HQ)
    left_cols = pl.ds(pl.multiple_of(xL * HQ, HQ), HQ)
    right_cols = pl.ds(pl.multiple_of(xR * HQ, HQ), HQ)
    far_cols = pl.ds(pl.multiple_of(xO * HQ, HQ), HQ)
    own_rows = pl.ds(pl.multiple_of(s * UQ, UQ), UQ)
    left_rows = pl.ds(pl.multiple_of(xL * UQ, UQ), UQ)
    right_rows = pl.ds(pl.multiple_of(xR * UQ, UQ), UQ)
    far_rows = pl.ds(pl.multiple_of(xO * UQ, UQ), UQ)

    def h_copy(k, n, cols, rows, dev):
        view = hid.at[k - 1, :, cols]
        small = hsb.at[k - 1, rows, :]
        return (
            remote(view, view, h1_ss.at[k - 1, n], h1_rs.at[k - 1, n], dev),
            remote(small, small, h1_ss.at[k - 1, 2 + n], h1_rs.at[k - 1, 2 + n], dev),
        )

    def stage3(k):
        for copy in x_first(k)[4:]:
            copy.wait_recv()
        for copy in x_second(k):
            copy.wait_recv()
        gate = xs[k - 1, s, 0].astype(f32) + xr1[k - 1, 3].astype(f32) + xr2[k - 1, 0].astype(f32)
        up = xs[k - 1, s, 1].astype(f32) + xr1[k - 1, 1].astype(f32) + xr2[k - 1, 1].astype(f32)
        hid[k - 1, :, own_cols] = (gate / (1.0 + jnp.exp(-gate)) * up).astype(bf16)
        sg = ss[k - 1, s, 0] + sr1[k - 1, 3] + sr2[k - 1, 0]
        su = ss[k - 1, s, 1] + sr1[k - 1, 1] + sr2[k - 1, 1]
        hsb[k - 1, own_rows, :] = sg / (1.0 + jnp.exp(-sg)) * su
        for copy in h_copy(k, 0, own_cols, own_rows, x_right) + h_copy(k, 1, own_cols, own_rows, x_left):
            copy.start()

    def h_far(k, n, cols, rows, dev):
        view = hid.at[k - 1, pl.ds(n * (R // 2), R // 2), cols]
        small = hsb.at[k - 1, rows, pl.ds(n * 2 * T, 2 * T)]
        return (
            remote(view, view, h2_ss.at[k - 1, n], h2_rs.at[k - 1, n], dev),
            remote(small, small, h2_ss.at[k - 1, 2 + n], h2_rs.at[k - 1, 2 + n], dev),
        )

    def stage4(k):
        for n, cols, rows, dev in ((0, left_cols, left_rows, x_right), (1, right_cols, right_rows, x_left)):
            for copy in h_copy(k, n, cols, rows, dev):
                copy.wait_recv()
            for copy in h_far(k, n, cols, rows, dev):
                copy.start()

    def give(k, d):
        return remote(ps.at[k - 1, d], pr.at[k - 1, d], pd_ss.at[k - 1, d], pd_rs.at[k - 1, d], partner)

    def stage5(k):
        for n, dev in ((0, x_right), (1, x_left)):
            for copy in h_far(k, n, far_cols, far_rows, dev):
                copy.wait_recv()
        lhs_t[k - 1, R : R + units, :] = hsb[k - 1].astype(bf16)
        both_t = lhs_t[k - 1]
        weight = jnp.sum(both_t[0:R].astype(f32) * wsel[k - 1, 0:1], axis=1, keepdims=True)
        both = jnp.transpose(both_t.astype(f32)).astype(bf16)
        hidden = hid[k - 1]

        o = jnp.dot(hidden, down_v[...], preferred_element_type=f32)
        o = (o * weight).astype(bf16)
        stacked = jnp.concatenate([o, sdown_ref[...]], axis=0)
        part = jnp.dot(both, stacked, preferred_element_type=f32)
        for d in (0, 1):
            con[k - 1, d] = part[2 * d * T : (2 * d + 1) * T]
            ps[k - 1, d] = part[(2 * d + 1) * T : (2 * d + 2) * T].astype(bf16)
        for d in (0, 1):
            give(k, d).start()

    def during(k, stage):
        @pl.when((k >= 1) & (k <= H))
        def _():
            stage(k)

    def step(t, _):
        forward(t, 0)
        forward(t, NC)

        @pl.when(t == 2)
        def _():
            for w in weights:
                w.wait()

        during(t - 1, stage1a)
        forward(t, 1)
        during(t - 1, stage1b)
        forward(t, 2)
        during(t - 5, stage5)
        forward(t, 3)
        during(t - 4, stage4)
        during(t - 3, stage3)
        during(t - 2, stage2)
        return 0

    lax.fori_loop(1, H + 6, step, 0)

    def rows(i):
        return pl.ds(i * CH, CH)

    def pass_on(m, d, i):
        return remote(
            rs_s.at[m, d - 1, rows(i)],
            rs_r.at[m, d - 1, rows(i)],
            r_ss.at[m, d - 1, i],
            r_rs.at[m, d - 1, i],
            z_next[m],
        )

    def own_sum(d, slot, i):
        return con[d - 1, slot, rows(i), :] + pr[d - 1, slot, rows(i), :].astype(f32)

    def drain(k):
        for i in range(NC + 1):
            for m in (0, 1):
                hand(m, k, i).wait_send()

                @pl.when(k < H)
                def _():
                    ring_arrival(m, k, i).wait_send()

                if mine(m, i):

                    @pl.when(k == H)
                    def _():
                        ring_arrival(m, k, i).wait_send()

        for copy in x_first(k) + x_second(k):
            copy.wait_send()
        for n, dev in ((0, x_right), (1, x_left)):
            for copy in h_copy(k, n, own_cols, own_rows, dev) + h_far(k, n, own_cols, own_rows, dev):
                copy.wait_send()
            give(k, n).wait_send()

    def drain_back(d):
        for i in range(NC):
            for m in (0, 1):

                @pl.when(d < H)
                def _():
                    pass_on(m, d, i).wait_send()

                if mine(m, i):

                    @pl.when(d == H)
                    def _():
                        pass_on(m, d, i).wait_send()

    give(H, 0).wait_recv()
    for i in range(NC):
        m = 0 if mine(0, i) else 1
        rs_s[m, H - 1, rows(i), :] = own_sum(H, 0, i).astype(bf16)
        pass_on(m, H, i).start()
    drain(H)

    def back(d, partly):
        give(d, 0).wait_recv()
        give(d, 1).wait_recv()
        for i in range(NC):
            for m in (0, 1):
                total = own_sum(d, 1 - m, i)
                if not partly or mine(m, i):
                    pass_on(m, d + 1, i).wait_recv()
                    total = total + rs_r[m, d, rows(i), :].astype(f32)
                rs_s[m, d - 1, rows(i), :] = total.astype(bf16)
                pass_on(m, d, i).start()
        drain(d)

    if H > 1:
        back(H - 1, True)

    def back_step(n, _):
        back(H - 2 - n, False)
        drain_back(H - n)
        return 0

    lax.fori_loop(0, H - 2, back_step, 0)
    give(H, 1).wait_recv()
    for i in range(NC):
        total = own_sum(H, 1, i)
        for m in (0, 1):
            pass_on(m, 1, i).wait_recv()
            total = total + rs_r[m, 0, rows(i), :].astype(f32)
        out_ref[rows(i), :] = total.astype(bf16)

    for d in range(1, min(3, H + 1)):
        drain_back(d)


def per_device(
    tokens,
    expert_ids,
    route_weights,
    gate_weight,
    up_weight,
    down_weight,
    shared_gate,
    shared_up,
    shared_down,
):
    f32, bf16 = jnp.float32, jnp.bfloat16
    nep = lax.axis_size("ep")
    nsub = lax.axis_size("sub")
    nz = nep // 2
    H = nz // 2
    T, Q = tokens.shape
    top = expert_ids.shape[1]
    cap = T * top * 3 // (2 * nep)
    units = shared_gate.shape[0]
    hidden = gate_weight.shape[2]
    HQ, UQ, R = hidden // nsub, units // nsub, 4 * cap
    vmem = pltpu.VMEM
    dma = pltpu.SemaphoreType.DMA
    vspec = pl.BlockSpec(memory_space=pltpu.VMEM)
    hspec = pl.BlockSpec(memory_space=pl.ANY)
    scratch = [vmem((units, Q), bf16)] * 3 + [
        vmem((Q, hidden), bf16),
        vmem((Q, hidden), bf16),
        vmem((hidden, Q), bf16),
        vmem((H, 4 * T, Q), bf16),
        vmem((H, 4, top, 2 * T), f32),
        vmem((R, Q), bf16),
        vmem((4 * T, 4 * T), bf16),
        vmem((H, R + units, 4 * T), bf16),
        vmem((H, 8, 4 * T), f32),
        vmem((H, nsub, 2, R, HQ), bf16),
        vmem((H, 4, R, HQ), bf16),
        vmem((H, 2, R, HQ), bf16),
        vmem((H, 2, R, HQ), bf16),
        vmem((H, nsub, 2, UQ, 4 * T), f32),
        vmem((H, 4, UQ, 4 * T), f32),
        vmem((H, 2, UQ, 4 * T), f32),
        vmem((H, 2, UQ, 4 * T), f32),
        vmem((H, R, hidden), bf16),
        vmem((H, units, 4 * T), f32),
        vmem((H, 2, T, Q), f32),
        vmem((H, 2, T, Q), bf16),
        vmem((H, 2, T, Q), bf16),
        vmem((2, H, T, Q), bf16),
        vmem((2, H, T, Q), bf16),
        dma((7,)),
    ]
    for shape in ((2, H, NC + 1), (2, H, NC + 1), (H, 8), (H, 4), (H, 4), (H, 4), (H, 2), (2, H, NC)):
        scratch += [dma(shape), dma(shape)]
    return pl.pallas_call(
        functools.partial(layer_kernel, (nz, nsub, cap, units)),
        out_shape=jax.ShapeDtypeStruct((T, Q), bf16),
        in_specs=[vspec] * 2 + [hspec] * 7,
        out_specs=vspec,
        scratch_shapes=scratch,
        compiler_params=pltpu.CompilerParams(
            collective_id=0, has_side_effects=True, vmem_limit_bytes=67043328
        ),
    )(
        expert_ids.T,
        route_weights.T,
        tokens,
        shared_gate,
        shared_up,
        shared_down,
        gate_weight[0],
        up_weight[0],
        down_weight[0],
    )


def solution(mesh):
    in_specs = (
        P(("groups", "ep"), "sub"),
        P(("groups", "ep"), None),
        P(("groups", "ep"), None),
        P("ep", "sub", None),
        P("ep", "sub", None),
        P("ep", None, "sub"),
        P("ep", "sub"),
        P("ep", "sub"),
        P("ep", "sub"),
    )
    out_specs = P(("groups", "ep"), "sub")
    return jax.shard_map(
        per_device, mesh=mesh, in_specs=in_specs, out_specs=out_specs, check_vma=False
    )
```

```python
import functools

import jax
import jax.numpy as jnp
from jax import lax
from jax.experimental import pallas as pl
from jax.experimental.pallas import tpu as pltpu
from jax.sharding import PartitionSpec as P

MESH = pl.DeviceIdType.MESH
NC = 4


def layer_kernel(
    dims,
    ids_ref,
    route_ref,
    tokens_hbm,
    sgate_hbm,
    sup_hbm,
    sdown_hbm,
    gate_hbm,
    up_hbm,
    down_hbm,
    out_ref,
    sgate_ref,
    sup_ref,
    sdown_ref,
    gate_v,
    up_v,
    down_v,
    tok,
    meta,
    comp,
    upper,
    lhs_t,
    wsel,
    xs,
    xr1,
    xc,
    xr2,
    ss,
    sr1,
    sc,
    sr2,
    hid,
    hsb,
    con,
    ps,
    pr,
    rs_s,
    rs_r,
    w_sem,
    ag_ss,
    ag_rs,
    dd_ss,
    dd_rs,
    x1_ss,
    x1_rs,
    x2_ss,
    x2_rs,
    h1_ss,
    h1_rs,
    h2_ss,
    h2_rs,
    pd_ss,
    pd_rs,
    r_ss,
    r_rs,
):
    nz, nsub, cap, units = dims
    f32, bf16 = jnp.float32, jnp.bfloat16
    H = nz // 2
    T, Q = tokens_hbm.shape
    CH = T // NC
    R = 4 * cap
    HQ = gate_v.shape[1] // nsub
    UQ = units // nsub
    TILE = 256
    ntile = Q // TILE

    e = lax.axis_index("ep")
    s = lax.axis_index("sub")
    z = e // 2
    c = e % 2
    z_right = {"ep": ((z + 1) % nz) * 2 + c}
    z_left = {"ep": ((z + nz - 1) % nz) * 2 + c}
    z_next = (z_right, z_left)
    partner = {"ep": z * 2 + (1 - c)}
    xR = (s + 1) % nsub
    xL = (s + nsub - 1) % nsub
    xO = (s + 2) % nsub
    x_right = {"sub": xR}
    x_left = {"sub": xL}

    def remote(src, dst, ssem, rsem, dev):
        return pltpu.make_async_remote_copy(
            src_ref=src, dst_ref=dst, send_sem=ssem, recv_sem=rsem, device_id=dev, device_id_type=MESH
        )

    weights = [
        pltpu.make_async_copy(a, b, w_sem.at[n])
        for n, (a, b) in enumerate(
            (
                (gate_hbm, gate_v),
                (up_hbm, up_v),
                (sgate_hbm, sgate_ref),
                (sup_hbm, sup_ref),
                (sdown_hbm, sdown_ref),
                (down_hbm, down_v),
            )
        )
    ]
    own_tokens = tok.at[H - 1, pl.ds(2 * T, T)]
    own_meta = meta.at[H - 1, 2]
    fetch = pltpu.make_async_copy(tokens_hbm, own_tokens, w_sem.at[6])
    fetch.start()
    own_meta[:, 0:T] = ids_ref[...].astype(f32)
    own_meta[:, T : 2 * T] = route_ref[...]

    barrier = pltpu.get_barrier_semaphore()
    for peer in (z_right, z_left, partner, x_right, x_left):
        pl.semaphore_signal(barrier, inc=1, device_id=peer, device_id_type=MESH)
    pl.semaphore_wait(barrier, 5)
    fetch.wait()

    def mine(m, i):
        return (i < NC // 2 or i == NC) if m == 0 else (NC // 2 <= i < NC)

    def slot_of(m, t):
        return m * (1 - t // H)

    def rows_of(d, rel, i):
        return pl.ds((2 * d + rel) * T + i * CH, CH)

    def ring(m, t, i, first=False):
        d = slot_of(m, t)
        if i == NC:
            src = own_meta if first else meta.at[t - 2, 2 * m]
            dst = meta.at[t - 1, 2 * d]
        else:
            src = own_tokens.at[pl.ds(i * CH, CH)] if first else tok.at[t - 2, rows_of(m, 0, i)]
            dst = tok.at[t - 1, rows_of(d, 0, i)]
        return remote(src, dst, ag_ss.at[m, t - 1, i], ag_rs.at[m, t - 1, i], z_next[m])

    def ring_arrival(m, t, i):
        d = slot_of(m, t)
        dst = meta.at[t - 1, 2 * d] if i == NC else tok.at[t - 1, rows_of(d, 0, i)]
        return remote(dst, dst, ag_ss.at[m, t - 1, i], ag_rs.at[m, t - 1, i], z_next[m])

    def hand(d, t, i, own=False):
        if i == NC:
            src = own_meta if own else meta.at[t - 1, 2 * d]
            dst = meta.at[t - 1, 2 * d + 1]
        else:
            src = own_tokens.at[pl.ds(i * CH, CH)] if own else tok.at[t - 1, rows_of(d, 0, i)]
            dst = tok.at[t - 1, rows_of(d, 1, i)]
        return remote(src, dst, dd_ss.at[d, t - 1, i], dd_rs.at[d, t - 1, i], partner)

    order = [0, NC] + list(range(1, NC))
    for i in order:
        for m in (0, 1):
            if H > 1 or mine(m, i):
                ring(m, 1, i, first=True).start()
    for i in order:
        hand(1, H, i, own=True).start()
    for w in weights:
        w.start()

    row_i = lax.broadcasted_iota(jnp.int32, (4 * T, 4 * T), 0)
    col_i = lax.broadcasted_iota(jnp.int32, (4 * T, 4 * T), 1)
    upper[...] = ((row_i < col_i) & (row_i // T == col_i // T)).astype(f32).astype(bf16)

    def forward(t, i):
        for m in (0, 1):

            @pl.when(t < H)
            def _():
                ring_arrival(m, t, i).wait_recv()
                if mine(m, i):
                    ring(m, t + 1, i).start()
                else:

                    @pl.when(t + 1 < H)
                    def _():
                        ring(m, t + 1, i).start()

                hand(m, t, i).start()

            if mine(m, i):

                @pl.when(t == H)
                def _():
                    ring_arrival(m, t, i).wait_recv()
                    hand(0, t, i).start()

    def stage1a(k):
        for d in (0, 1):
            for i in range(NC + 1):
                hand(d, k, i).wait_recv()
        half = lax.broadcasted_iota(jnp.int32, own_meta.shape, 1) < T
        ids, ws = [], []
        for d in (0, 1):
            m0 = meta[k - 1, 2 * d]
            m1 = meta[k - 1, 2 * d + 1]
            ids.append(jnp.where(half, m0, pltpu.roll(m1, T, 1)))
            ws.append(jnp.where(half, pltpu.roll(m0, T, 1), m1))
        ids = jnp.concatenate(ids, axis=1)
        ws = jnp.concatenate(ws, axis=1)
        hit = ids == e.astype(f32)
        sel = jnp.max(jnp.where(hit, 1.0, 0.0), axis=0, keepdims=True)
        wsel[k - 1] = jnp.broadcast_to(
            jnp.sum(jnp.where(hit, ws, 0.0), axis=0, keepdims=True), (8, 4 * T)
        )
        sel8 = jnp.broadcast_to(sel, (16, 4 * T)).astype(bf16)
        pos = jnp.dot(sel8, upper[...], preferred_element_type=f32)[0:1]
        base = (lax.broadcasted_iota(jnp.int32, (1, 4 * T), 1) // T * cap).astype(f32)
        target = jnp.where(sel > 0.0, pos + base, -1.0)
        place = lax.broadcasted_iota(jnp.int32, (R, 4 * T), 0).astype(f32) == target
        place = jnp.where(place, 1.0, 0.0).astype(bf16)
        lhs_t[k - 1, 0:R, :] = place

        comp[...] = jnp.dot(place, tok[k - 1], preferred_element_type=f32).astype(bf16)

    def x_first(k):
        return (
            remote(xs.at[k - 1, xO, 0], xr1.at[k - 1, 0], x1_ss.at[k - 1, 0], x1_rs.at[k - 1, 0], x_right),
            remote(xs.at[k - 1, xO, 1], xr1.at[k - 1, 2], x1_ss.at[k - 1, 2], x1_rs.at[k - 1, 2], x_left),
            remote(ss.at[k - 1, xO, 0], sr1.at[k - 1, 0], x1_ss.at[k - 1, 4], x1_rs.at[k - 1, 4], x_right),
            remote(ss.at[k - 1, xO, 1], sr1.at[k - 1, 2], x1_ss.at[k - 1, 6], x1_rs.at[k - 1, 6], x_left),
            remote(xs.at[k - 1, xR, 1], xr1.at[k - 1, 1], x1_ss.at[k - 1, 1], x1_rs.at[k - 1, 1], x_right),
            remote(xs.at[k - 1, xL, 0], xr1.at[k - 1, 3], x1_ss.at[k - 1, 3], x1_rs.at[k - 1, 3], x_left),
            remote(ss.at[k - 1, xR, 1], sr1.at[k - 1, 1], x1_ss.at[k - 1, 5], x1_rs.at[k - 1, 5], x_right),
            remote(ss.at[k - 1, xL, 0], sr1.at[k - 1, 3], x1_ss.at[k - 1, 7], x1_rs.at[k - 1, 7], x_left),
        )

    def stage1b(k):
        rows = comp[...]

        first = x_first(k)
        ga = jnp.dot(rows, gate_v[...], preferred_element_type=f32).astype(bf16)
        for j in range(nsub):
            xs[k - 1, j, 0] = ga[:, j * HQ : (j + 1) * HQ]
        first[0].start()
        ua = jnp.dot(rows, up_v[...], preferred_element_type=f32).astype(bf16)
        for j in range(nsub):
            xs[k - 1, j, 1] = ua[:, j * HQ : (j + 1) * HQ]
        first[1].start()
        contract = (((1,), (1,)), ((), ()))
        pre = lax.dot_general(sgate_ref[...], tok[k - 1], contract, preferred_element_type=f32)
        lin = lax.dot_general(sup_ref[...], tok[k - 1], contract, preferred_element_type=f32)
        for j in range(nsub):
            ss[k - 1, j, 0] = pre[j * UQ : (j + 1) * UQ]
            ss[k - 1, j, 1] = lin[j * UQ : (j + 1) * UQ]
        for copy in first[2:]:
            copy.start()

    def x_second(k):
        return (
            remote(xc.at[k - 1, 0], xr2.at[k - 1, 0], x2_ss.at[k - 1, 0], x2_rs.at[k - 1, 0], x_right),
            remote(xc.at[k - 1, 1], xr2.at[k - 1, 1], x2_ss.at[k - 1, 1], x2_rs.at[k - 1, 1], x_left),
            remote(sc.at[k - 1, 0], sr2.at[k - 1, 0], x2_ss.at[k - 1, 2], x2_rs.at[k - 1, 2], x_right),
            remote(sc.at[k - 1, 1], sr2.at[k - 1, 1], x2_ss.at[k - 1, 3], x2_rs.at[k - 1, 3], x_left),
        )

    def stage2(k):
        first = x_first(k)
        second = x_second(k)
        for m, toward in ((0, xR), (1, xL)):
            first[m].wait_recv()
            xc[k - 1, m] = (
                xs[k - 1, toward, m].astype(f32) + xr1[k - 1, 2 * m].astype(f32)
            ).astype(bf16)
            second[m].start()
        for m, toward in ((0, xR), (1, xL)):
            first[2 + m].wait_recv()
            sc[k - 1, m] = ss[k - 1, toward, m] + sr1[k - 1, 2 * m]
            second[2 + m].start()

    own_cols = pl.ds(pl.multiple_of(s * HQ, HQ), HQ)
    left_cols = pl.ds(pl.multiple_of(xL * HQ, HQ), HQ)
    right_cols = pl.ds(pl.multiple_of(xR * HQ, HQ), HQ)
    far_cols = pl.ds(pl.multiple_of(xO * HQ, HQ), HQ)
    own_rows = pl.ds(pl.multiple_of(s * UQ, UQ), UQ)
    left_rows = pl.ds(pl.multiple_of(xL * UQ, UQ), UQ)
    right_rows = pl.ds(pl.multiple_of(xR * UQ, UQ), UQ)
    far_rows = pl.ds(pl.multiple_of(xO * UQ, UQ), UQ)

    def h_copy(k, n, cols, rows, dev):
        view = hid.at[k - 1, :, cols]
        small = hsb.at[k - 1, rows, :]
        return (
            remote(view, view, h1_ss.at[k - 1, n], h1_rs.at[k - 1, n], dev),
            remote(small, small, h1_ss.at[k - 1, 2 + n], h1_rs.at[k - 1, 2 + n], dev),
        )

    def stage3(k):
        for copy in x_first(k)[4:]:
            copy.wait_recv()
        for copy in x_second(k):
            copy.wait_recv()
        gate = xs[k - 1, s, 0].astype(f32) + xr1[k - 1, 3].astype(f32) + xr2[k - 1, 0].astype(f32)
        up = xs[k - 1, s, 1].astype(f32) + xr1[k - 1, 1].astype(f32) + xr2[k - 1, 1].astype(f32)
        hid[k - 1, :, own_cols] = (gate / (1.0 + jnp.exp(-gate)) * up).astype(bf16)
        sg = ss[k - 1, s, 0] + sr1[k - 1, 3] + sr2[k - 1, 0]
        su = ss[k - 1, s, 1] + sr1[k - 1, 1] + sr2[k - 1, 1]
        hsb[k - 1, own_rows, :] = sg / (1.0 + jnp.exp(-sg)) * su
        for copy in h_copy(k, 0, own_cols, own_rows, x_right) + h_copy(k, 1, own_cols, own_rows, x_left):
            copy.start()

    def h_far(k, n, cols, rows, dev):
        view = hid.at[k - 1, pl.ds(n * (R // 2), R // 2), cols]
        small = hsb.at[k - 1, rows, pl.ds(n * 2 * T, 2 * T)]
        return (
            remote(view, view, h2_ss.at[k - 1, n], h2_rs.at[k - 1, n], dev),
            remote(small, small, h2_ss.at[k - 1, 2 + n], h2_rs.at[k - 1, 2 + n], dev),
        )

    def stage4(k):
        for n, cols, rows, dev in ((0, left_cols, left_rows, x_right), (1, right_cols, right_rows, x_left)):
            for copy in h_copy(k, n, cols, rows, dev):
                copy.wait_recv()
            for copy in h_far(k, n, cols, rows, dev):
                copy.start()

    def give(k, d):
        return remote(ps.at[k - 1, d], pr.at[k - 1, d], pd_ss.at[k - 1, d], pd_rs.at[k - 1, d], partner)

    def stage5(k):
        for n, dev in ((0, x_right), (1, x_left)):
            for copy in h_far(k, n, far_cols, far_rows, dev):
                copy.wait_recv()
        lhs_t[k - 1, R : R + units, :] = hsb[k - 1].astype(bf16)
        both_t = lhs_t[k - 1]
        weight = jnp.sum(both_t[0:R].astype(f32) * wsel[k - 1, 0:1], axis=1, keepdims=True)
        both = jnp.transpose(both_t.astype(f32)).astype(bf16)
        hidden = hid[k - 1]

        o = jnp.dot(hidden, down_v[...], preferred_element_type=f32)
        o = (o * weight).astype(bf16)
        stacked = jnp.concatenate([o, sdown_ref[...]], axis=0)
        part = jnp.dot(both, stacked, preferred_element_type=f32)
        for d in (0, 1):
            con[k - 1, d] = part[2 * d * T : (2 * d + 1) * T]
            ps[k - 1, d] = part[(2 * d + 1) * T : (2 * d + 2) * T].astype(bf16)
        for d in (0, 1):
            give(k, d).start()

    def during(k, stage):
        @pl.when((k >= 1) & (k <= H))
        def _():
            stage(k)

    def step(t, _):
        forward(t, 0)
        forward(t, NC)

        @pl.when(t == 2)
        def _():
            for w in weights:
                w.wait()

        during(t - 1, stage1a)
        forward(t, 1)
        during(t - 1, stage1b)
        forward(t, 2)
        forward(t, 3)
        during(t - 4, stage4)
        during(t - 3, stage3)
        during(t - 2, stage2)
        during(t - 5, stage5)
        return 0

    lax.fori_loop(1, H + 6, step, 0)

    def rows(i):
        return pl.ds(i * CH, CH)

    def pass_on(m, d, i):
        return remote(
            rs_s.at[m, d - 1, rows(i)],
            rs_r.at[m, d - 1, rows(i)],
            r_ss.at[m, d - 1, i],
            r_rs.at[m, d - 1, i],
            z_next[m],
        )

    def own_sum(d, slot, i):
        return con[d - 1, slot, rows(i), :] + pr[d - 1, slot, rows(i), :].astype(f32)

    def drain(k):
        for i in range(NC + 1):
            for m in (0, 1):
                hand(m, k, i).wait_send()

                @pl.when(k < H)
                def _():
                    ring_arrival(m, k, i).wait_send()

                if mine(m, i):

                    @pl.when(k == H)
                    def _():
                        ring_arrival(m, k, i).wait_send()

        for copy in x_first(k) + x_second(k):
            copy.wait_send()
        for n, dev in ((0, x_right), (1, x_left)):
            for copy in h_copy(k, n, own_cols, own_rows, dev) + h_far(k, n, own_cols, own_rows, dev):
                copy.wait_send()
            give(k, n).wait_send()

    def drain_back(d):
        for i in range(NC):
            for m in (0, 1):

                @pl.when(d < H)
                def _():
                    pass_on(m, d, i).wait_send()

                if mine(m, i):

                    @pl.when(d == H)
                    def _():
                        pass_on(m, d, i).wait_send()

    give(H, 0).wait_recv()
    for i in range(NC):
        m = 0 if mine(0, i) else 1
        rs_s[m, H - 1, rows(i), :] = own_sum(H, 0, i).astype(bf16)
        pass_on(m, H, i).start()
    drain(H)

    def back(d, partly):
        give(d, 0).wait_recv()
        give(d, 1).wait_recv()
        for i in range(NC):
            for m in (0, 1):
                total = own_sum(d, 1 - m, i)
                if not partly or mine(m, i):
                    pass_on(m, d + 1, i).wait_recv()
                    total = total + rs_r[m, d, rows(i), :].astype(f32)
                rs_s[m, d - 1, rows(i), :] = total.astype(bf16)
                pass_on(m, d, i).start()
        drain(d)

    if H > 1:
        back(H - 1, True)

    def back_step(n, _):
        back(H - 2 - n, False)
        drain_back(H - n)
        return 0

    lax.fori_loop(0, H - 2, back_step, 0)
    give(H, 1).wait_recv()
    for i in range(NC):
        total = own_sum(H, 1, i)
        for m in (0, 1):
            pass_on(m, 1, i).wait_recv()
            total = total + rs_r[m, 0, rows(i), :].astype(f32)
        out_ref[rows(i), :] = total.astype(bf16)

    for d in range(1, min(3, H + 1)):
        drain_back(d)


def per_device(
    tokens,
    expert_ids,
    route_weights,
    gate_weight,
    up_weight,
    down_weight,
    shared_gate,
    shared_up,
    shared_down,
):
    f32, bf16 = jnp.float32, jnp.bfloat16
    nep = lax.axis_size("ep")
    nsub = lax.axis_size("sub")
    nz = nep // 2
    H = nz // 2
    T, Q = tokens.shape
    top = expert_ids.shape[1]
    cap = T * top * 3 // (2 * nep)
    units = shared_gate.shape[0]
    hidden = gate_weight.shape[2]
    HQ, UQ, R = hidden // nsub, units // nsub, 4 * cap
    vmem = pltpu.VMEM
    dma = pltpu.SemaphoreType.DMA
    vspec = pl.BlockSpec(memory_space=pltpu.VMEM)
    hspec = pl.BlockSpec(memory_space=pl.ANY)
    scratch = [vmem((units, Q), bf16)] * 3 + [
        vmem((Q, hidden), bf16),
        vmem((Q, hidden), bf16),
        vmem((hidden, Q), bf16),
        vmem((H, 4 * T, Q), bf16),
        vmem((H, 4, top, 2 * T), f32),
        vmem((R, Q), bf16),
        vmem((4 * T, 4 * T), bf16),
        vmem((H, R + units, 4 * T), bf16),
        vmem((H, 8, 4 * T), f32),
        vmem((H, nsub, 2, R, HQ), bf16),
        vmem((H, 4, R, HQ), bf16),
        vmem((H, 2, R, HQ), bf16),
        vmem((H, 2, R, HQ), bf16),
        vmem((H, nsub, 2, UQ, 4 * T), f32),
        vmem((H, 4, UQ, 4 * T), f32),
        vmem((H, 2, UQ, 4 * T), f32),
        vmem((H, 2, UQ, 4 * T), f32),
        vmem((H, R, hidden), bf16),
        vmem((H, units, 4 * T), f32),
        vmem((H, 2, T, Q), f32),
        vmem((H, 2, T, Q), bf16),
        vmem((H, 2, T, Q), bf16),
        vmem((2, H, T, Q), bf16),
        vmem((2, H, T, Q), bf16),
        dma((7,)),
    ]
    for shape in ((2, H, NC + 1), (2, H, NC + 1), (H, 8), (H, 4), (H, 4), (H, 4), (H, 2), (2, H, NC)):
        scratch += [dma(shape), dma(shape)]
    return pl.pallas_call(
        functools.partial(layer_kernel, (nz, nsub, cap, units)),
        out_shape=jax.ShapeDtypeStruct((T, Q), bf16),
        in_specs=[vspec] * 2 + [hspec] * 7,
        out_specs=vspec,
        scratch_shapes=scratch,
        compiler_params=pltpu.CompilerParams(
            collective_id=0, has_side_effects=True, vmem_limit_bytes=67043328
        ),
    )(
        expert_ids.T,
        route_weights.T,
        tokens,
        shared_gate,
        shared_up,
        shared_down,
        gate_weight[0],
        up_weight[0],
        down_weight[0],
    )


def solution(mesh):
    in_specs = (
        P(("groups", "ep"), "sub"),
        P(("groups", "ep"), None),
        P(("groups", "ep"), None),
        P("ep", "sub", None),
        P("ep", "sub", None),
        P("ep", None, "sub"),
        P("ep", "sub"),
        P("ep", "sub"),
        P("ep", "sub"),
    )
    out_specs = P(("groups", "ep"), "sub")
    return jax.shard_map(
        per_device, mesh=mesh, in_specs=in_specs, out_specs=out_specs, check_vma=False
    )
```
